512 devices in a mesh: seq: 32 (over x, y), head: 16 (over z, core).
Axes of the slice: x: 4, y: 8, z: 8, core: 2. Of those that a mesh axis runs over, the one named last changes fastest.
Arguments:
- projected: bfloat16 [3, 4096, 2048], P(None, 'seq', 'head'), may hold values from -6 to 6
- out_grad: bfloat16 [4096, 2048], P('seq', 'head'), may hold values from -6 to 6
- logits: float32 [2, 16, 4096], P(None, 'head', 'seq'), may hold values from -6 to 6
- head_params: float32 [2, 16], P(None, 'head'), may hold values from -12 to 1, as said below
- qkv_weight: bfloat16 [3, 2048, 2048], P(None, None, 'head'), may hold values from -0.1875 to 0.1875
- gate_weight: bfloat16 [2, 16, 2048], P(None, 'head'), may hold values from -1.5 to 1.5
Outputs:
- input_grad: bfloat16 [4096, 2048], P('seq', 'head')
The draws below stay inside these ranges and needn't reach their ends.
Inputs may be any that keep to these rules, and one draw needn't show every extreme that they name: `head_params`: row 0 holds the logarithms of the heads' decay scales, row 1 the decay biases.
All inputs are finite; a program needn't handle non-finite values.
Results may differ from the reference program's by a relative error of at most 0.0034.
Values sent between devices are 32-bit elements; how exact they have to be, the bound alone decides.
No kernel may reach another device: no remote copies, remote signals or barrier semaphores. Data moves between devices by JAX's collectives and lax.ppermute only.
A program may use at most 64 MiB of HBM per device.

```python
import math
import jax
import jax.numpy as jnp
from jax import lax

D = 2048
DK = 128
H = 16
BLOCK = 64
TOKENS = 4096


def draw_head_params(key, part):
    rate_key, bias_key = jax.random.split(jax.random.fold_in(key, 17))
    rates = jax.random.uniform(rate_key, (H,), jnp.float32, math.log(0.0001), math.log(0.05))
    biases = jax.random.uniform(bias_key, (H,), jnp.float32, -1.0, 1.0)
    return jnp.stack([rates, biases])


def spiked(values, own_key, source, target, shards_of, factor):
    owner, partner = [(jnp.arange(values.shape[position]) // (values.shape[position] // shards_of)).reshape([-1 if axis == position else 1 for axis in range(values.ndim)]) for position in (source, target)]
    chosen = jax.random.permutation(own_key, shards_of)[partner]
    strong = (owner == chosen) | (owner == (partner + shards_of // 2) % shards_of)
    return jnp.where(strong, factor * values, values)


def level_of(stream_key, dims, cuts, least, top_value):
    factor_of, own = 1.0, jax.random.fold_in(stream_key, 6)
    for dim, parts in cuts:
        heights = jnp.exp(jax.random.uniform(jax.random.fold_in(own, dim), (parts,), jnp.float32, least / len(cuts), top_value / len(cuts)))
        factor_of = factor_of * jnp.repeat(heights, dims[dim] // parts).reshape([-1 if axis == dim else 1 for axis in range(len(dims))])
    return factor_of


def gaussian(key, extent, scale, limit, pieces=(), dtype=jnp.bfloat16):
    entries = jax.random.normal(key, extent, jnp.float32) * scale
    if len(pieces) > 0:
        entries = level_of(key, extent, pieces, -0.22, 0.18) * entries
    return jnp.clip(entries, min=-limit, max=limit).astype(dtype)


def gaussian_with(own_key, shape, width, bound, cuts, heavy, dtype=jnp.bfloat16):
    result = width * jax.random.normal(own_key, shape, jnp.float32)
    if cuts:
        result = result * level_of(own_key, shape, cuts, -0.22, 0.18)
    return jnp.clip(spiked(result, jax.random.fold_in(own_key, 3), *heavy), -bound, bound).astype(dtype)


def setup_inputs(seed: int = 0) -> dict:
    splits = jax.random.split(jax.random.key(seed), 7)
    projected = gaussian(splits[0], (3, TOKENS, H * DK), 1.0, 6.0, ((1, 32), (2, 16)))
    out_grad = gaussian(splits[1], (TOKENS, H * DK), 1.0, 6.0, ((0, 32), (1, 16)))
    logits = gaussian(splits[2], (2, H, TOKENS), 1.5, 6.0, ((1, 16), (2, 32)), jnp.float32)
    head_params = draw_head_params(jax.random.fold_in(splits[6], 71), 0)
    qkv_weight = gaussian_with(splits[4], (3, D, H * DK), D ** -0.5, 0.1875, ((2, 16),), (2, 1, 16, 2.0))
    gate_weight = gaussian(splits[5], (2, H, D), 0.25, 1.5, ((1, 16),))
    return dict(projected=projected, out_grad=out_grad, logits=logits, head_params=head_params, qkv_weight=qkv_weight, gate_weight=gate_weight)


exact_precision = lax.Precision.HIGHEST

def unit_rows(raw_rows):
    return raw_rows * lax.rsqrt(lax.optimization_barrier(jnp.sum(raw_rows * raw_rows, axis=-1, keepdims=True)) + 1.0)

def recurrence(query_raw, key_raw, values, logits, head_params):
    queries = unit_rows(query_raw) * DK ** (-0.5)
    keys = unit_rows(key_raw)
    decay = -jnp.exp(head_params[0])[:, None] * jax.nn.softplus(logits[0] + head_params[1][:, None])
    keep_gate = jnp.exp(decay).T
    write_gate = jax.nn.sigmoid(logits[1]).T
    blocks = TOKENS // BLOCK

    def shape_blocks(array):
        return array.reshape((blocks, BLOCK) + array.shape[1:])
    inputs = tuple((shape_blocks(array) for array in (queries, keys, values, keep_gate, write_gate)))

    def token_step(running_state, token_item):
        single_query_row, single_key_row, value_row, keep_row, write_row = token_item
        retrieved_values = jnp.einsum('xw,xwt->xt', single_key_row, running_state, precision=exact_precision)
        erased = running_state - write_row[:, None, None] * single_key_row[:, :, None] * retrieved_values[:, None, :]
        running_state = keep_row[:, None, None] * erased + write_row[:, None, None] * single_key_row[:, :, None] * value_row[:, None, :]
        return (running_state, jnp.einsum('xw,xwt->xt', single_query_row, running_state, precision=exact_precision))

    @jax.checkpoint
    def block_step(running_state, block_item):
        return lax.scan(token_step, running_state, block_item)
    start_state = jnp.zeros((H, DK, DK), jnp.float32)
    final_state, outputs = lax.scan(block_step, start_state, inputs)
    return outputs.reshape(TOKENS, H, DK)

def reference(projected, out_grad, logits, head_params, qkv_weight, gate_weight):
    raw_inputs = projected.astype(jnp.float32).reshape(3, TOKENS, H, DK)
    out_cotan = out_grad.astype(jnp.float32).reshape(TOKENS, H, DK)

    def forward_fn(query_raw, key_raw, values, logit_rows):
        return recurrence(query_raw, key_raw, values, logit_rows, head_params)
    outputs, pull_back = jax.vjp(forward_fn, raw_inputs[0], raw_inputs[1], raw_inputs[2], logits)
    query_grad, key_grad, value_grad, logit_grad = pull_back(out_cotan)
    stacked_gradient = jnp.stack([query_grad, key_grad, value_grad]).reshape(3, TOKENS, H * DK).astype(jnp.bfloat16)
    total_grad = jnp.zeros((TOKENS, D), jnp.float32)
    for source in range(3):
        total_grad = total_grad + lax.dot_general(stacked_gradient[source], qkv_weight[source], (((1,), (1,)), ((), ())), preferred_element_type=jnp.float32)
    total_grad = total_grad + jnp.einsum('jht,jhd->td', logit_grad, gate_weight.astype(jnp.float32), precision=exact_precision)
    return total_grad.astype(jnp.bfloat16)
```

```python
import jax
import jax.numpy as jnp
from jax import lax
from jax.experimental import pallas as pl
from jax.experimental.pallas import tpu as pltpu
from jax.sharding import Mesh
from jax.sharding import PartitionSpec as P

DK = 128
TOK = 128
ROWS = 4
COLS = 8
SLICE = DK // COLS
SCALE = DK ** (-0.5)
F32 = jnp.float32

NN = (((1,), (0,)), ((), ()))
NT = (((1,), (1,)), ((), ()))
TN = (((0,), (0,)), ((), ()))


BF16 = jnp.bfloat16


def halves(x):
    if isinstance(x, tuple):
        return x
    high = x.astype(BF16)
    return high, (x - high.astype(F32)).astype(BF16)


def dot(left, right, dims=NN):
    (lh, ll), (rh, rl) = halves(left), halves(right)

    def one(a, b):
        return lax.dot_general(a, b, dims, preferred_element_type=F32)

    return one(lh, rh) + (one(lh, rl) + one(ll, rh))


def iotas():
    row = lax.broadcasted_iota(jnp.int32, (TOK, TOK), 0)
    col = lax.broadcasted_iota(jnp.int32, (TOK, TOK), 1)
    return row, col


def lane_sum(x):
    return jnp.sum(x, axis=1, keepdims=True)


def unit(raw):
    scale = lax.rsqrt(lane_sum(raw * raw) + 1.0)
    return raw * scale, scale


def gates(logit_ref, head_ref, row, col):
    rate = jnp.exp(jnp.full((1, TOK), head_ref[0, 0], F32))
    shifted = logit_ref[0] + head_ref[1, 0]
    soft = jnp.maximum(shifted, 0.0) + jnp.log1p(jnp.exp(-jnp.abs(shifted)))
    decay_row = -rate * soft
    cumul = lane_sum(jnp.where(col <= row, decay_row, 0.0))
    cumul_row = jnp.sum(jnp.where(row == col, cumul, 0.0), axis=0, keepdims=True)
    last = cumul_row[:, TOK - 1 :]
    write = lane_sum(jnp.where(row == col, jax.nn.sigmoid(logit_ref[1]), 0.0))
    lower = row >= col
    ratio = jnp.where(lower, jnp.exp(jnp.where(lower, cumul - cumul_row, 0.0)), 0.0)
    slope = lane_sum(jnp.where(row == col, -rate * jax.nn.sigmoid(shifted), 0.0))
    return jnp.exp(cumul), jnp.exp(last - cumul), jnp.exp(last), write, ratio, slope


def inverse_of(strict, row, col):
    eye = jnp.where(row == col, 1.0, 0.0).astype(F32)
    near = jnp.where((row >> 3) == (col >> 3), strict, 0.0)
    power2 = dot(near, near)
    out = eye - near
    both = dot(jnp.concatenate([out, power2], 0), power2)
    out, power4 = out + both[:TOK], both[TOK:]
    out = out + dot(out, power4)
    for level in (3, 4, 5, 6):
        joined = ((row >> (level + 1)) == (col >> (level + 1))) & ((row >> level) != (col >> level))
        off = jnp.where(joined, strict, 0.0)
        pair = halves(out)
        out = out - dot(pair, dot(off, pair))
    return out


def chunk_kernel(proj_ref, grad_ref, logit_ref, head_ref, out_ref, saved_ref):
    row, col = iotas()
    grown, rest, total, write, ratio, _ = gates(logit_ref, head_ref, row, col)
    queries = unit(proj_ref[0].astype(F32))[0] * SCALE
    keys = unit(proj_ref[1].astype(F32))[0]
    values = proj_ref[2].astype(F32)
    out_grad = grad_ref[...].astype(F32)
    inner = dot(jnp.concatenate([keys, queries], 0), keys, NT)
    bare = jnp.where(row > col, ratio * inner[:TOK], 0.0)
    attend = ratio * inner[TOK:]
    inverse = inverse_of(bare * write, row, col)
    solved = dot(inverse, jnp.concatenate([(write * grown) * keys, write * values], 1))
    key_weights, base = solved[:, :DK], solved[:, DK:]
    rest_keys = rest * keys
    moved = dot(solved, rest_keys, TN)
    eye = jnp.where(row == col, 1.0, 0.0).astype(F32)
    step = total * eye - moved[:DK]
    offset = moved[DK:]
    back = dot(out_grad, grown * queries - dot(attend, key_weights), TN)
    for peer in range(COLS):
        out_ref[peer, :DK] = step
        out_ref[peer, DK : DK + SLICE] = offset[peer * SLICE : (peer + 1) * SLICE]
        out_ref[peer, DK + SLICE :] = back[peer * SLICE : (peer + 1) * SLICE]
    saved_ref[0] = inverse.T
    saved_ref[1] = key_weights
    saved_ref[2] = base
    saved_ref[3] = attend
    saved_ref[4] = bare
    saved_ref[5] = dot(attend, out_grad, TN)


def row_kernel(in_ref, out_ref, own_ref, scratch_ref):
    here_x = lax.axis_index("x")
    here_y = lax.axis_index("y")
    step = [in_ref[j, :DK] for j in range(COLS)]
    ahead = [in_ref[j, DK : DK + SLICE] for j in range(COLS)]
    back = [in_ref[j, DK + SLICE :] for j in range(COLS)]

    def joined(first, second):
        both = dot(jnp.concatenate([first[0], first[1]], 0), second[0])
        return (both[:DK], both[DK:] + second[1], first[2] + dot(second[2], first[0], NT))

    ones = list(zip(step, ahead, back))
    pairs = [joined(ones[2 * i], ones[2 * i + 1]) for i in range(4)]
    quads = [joined(pairs[2 * i], pairs[2 * i + 1]) for i in range(2)]
    whole = joined(quads[0], quads[1])

    zero = jnp.zeros((SLICE, DK), F32)
    b4 = quads[0][1]
    b2 = pairs[0][1]
    b6 = dot(b4, pairs[2][0]) + pairs[2][1]
    prefix = [
        zero,
        ahead[0],
        b2,
        dot(b2, step[2]) + ahead[2],
        b4,
        dot(b4, step[4]) + ahead[4],
        b6,
        dot(b6, step[6]) + ahead[6],
    ]
    c3 = quads[1][2]
    c5 = pairs[3][2]
    c1 = dot(c3, pairs[1][0], NT) + pairs[1][2]
    suffix = [
        dot(c1, step[1], NT) + back[1],
        c1,
        dot(c3, step[3], NT) + back[3],
        c3,
        dot(c5, step[5], NT) + back[5],
        c5,
        back[7],
        zero,
    ]

    row, col = iotas()
    eye = jnp.where(row == col, 1.0, 0.0).astype(F32)
    at_y = jnp.full((DK, DK), here_y, jnp.int32)
    high = at_y >= 4
    mid = (at_y & 2) != 0
    low = (at_y & 1) != 0
    before = jnp.where(high, quads[0][0], eye)
    before = dot(before, jnp.where(mid, jnp.where(high, pairs[2][0], pairs[0][0]), eye))
    single = in_ref[jnp.maximum(here_y - 1, 0), :DK]
    own_ref[0] = dot(before, jnp.where(low, single, eye))
    after = jnp.where(high, eye, quads[1][0])
    after = dot(jnp.where(mid, eye, jnp.where(high, pairs[3][0], pairs[1][0])), after)
    single = in_ref[jnp.minimum(here_y + 1, COLS - 1), :DK]
    own_ref[1] = dot(jnp.where(low, eye, single), after)

    scratch_ref[...] = whole[0]
    piece = scratch_ref[pl.ds(pl.multiple_of(here_y * SLICE, SLICE), SLICE)]
    for peer_x in range(ROWS):
        own = jnp.full((SLICE, DK), here_x, jnp.int32) == peer_x
        for peer_y in range(COLS):
            slot = peer_x * COLS + peer_y
            out_ref[slot, :SLICE] = piece
            out_ref[slot, SLICE : 2 * SLICE] = jnp.where(own, prefix[peer_y], whole[1])
            out_ref[slot, 2 * SLICE :] = jnp.where(own, suffix[peer_y], whole[2])


def grad_kernel(
    proj_ref,
    grad_ref,
    logit_ref,
    head_ref,
    weight_hbm,
    gate_ref,
    saved_ref,
    own_ref,
    in_ref,
    keep_ref,
    send_ref,
    weight_ref,
    sem,
):
    fetch = pltpu.make_async_copy(weight_hbm, weight_ref, sem)
    fetch.start()
    here_x = lax.axis_index("x")
    here_c = lax.axis_index("c")

    def part(row_at, kind):
        rows = pl.ds(row_at * COLS, COLS)
        return in_ref[rows, kind * SLICE : (kind + 1) * SLICE].reshape(DK, DK)

    step1, step2 = part(1, 0), part(2, 0)
    s1 = part(0, 1)
    s2 = dot(s1, step1) + part(1, 1)
    s3 = dot(s2, step2) + part(2, 1)
    g2 = part(3, 2)
    g1 = dot(g2, step2, NT) + part(2, 2)
    g0 = dot(g1, step1, NT) + part(1, 2)
    zero = jnp.zeros((DK, DK), F32)
    s_row = jnp.where(here_x == 0, zero, jnp.where(here_x == 1, s1, jnp.where(here_x == 2, s2, s3)))
    g_row = jnp.where(here_x == 3, zero, jnp.where(here_x == 2, g2, jnp.where(here_x == 1, g1, g0)))
    state = dot(s_row, own_ref[0]) + part(here_x, 1)
    later = dot(g_row, own_ref[1], NT) + part(here_x, 2)

    row, col = iotas()
    grown, rest, total, write, ratio, slope = gates(logit_ref, head_ref, row, col)
    q_unit, q_scale = unit(proj_ref[0].astype(F32))
    queries = q_unit * SCALE
    keys, k_scale = unit(proj_ref[1].astype(F32))
    values = proj_ref[2].astype(F32)
    out_grad = grad_ref[...].astype(F32)
    rest_keys = rest * keys
    attend = saved_ref[3]
    bare = saved_ref[4]

    fresh = saved_ref[2] - dot(saved_ref[1], state, NT)
    d_fresh = saved_ref[5] + dot(rest_keys, later, NT)
    pulled = dot(saved_ref[0], d_fresh)
    both = dot(jnp.concatenate([out_grad, pulled], 0), state)
    d_query_decayed = both[:TOK]
    d_weighted = -both[TOK:]
    d_rest = dot(fresh, later)
    both = dot(jnp.concatenate([out_grad, pulled], 0), fresh, NT)
    d_attend = jnp.where(row >= col, both[:TOK], 0.0)
    d_lower = jnp.where(row > col, -both[TOK:], 0.0)
    d_qk = d_attend * ratio
    d_kk = d_lower * ratio * write
    stacked = jnp.concatenate([d_qk, d_kk], 0)
    by_key = dot(stacked, keys)
    across = dot(stacked, jnp.concatenate([queries, keys], 0), TN)
    d_queries = grown * d_query_decayed + by_key[:TOK]
    d_keys = by_key[TOK:] + across + rest * d_rest + (write * grown) * d_weighted

    lower_hit = d_lower * bare
    ratio_hit = d_attend * attend + lower_hit * write
    weighted_hit = grown * lane_sum(d_weighted * keys)
    rest_hit = lane_sum(d_rest * rest_keys)
    d_write = lane_sum(pulled * values) + weighted_hit + lane_sum(lower_hit)
    d_cumul = (
        lane_sum(ratio_hit)
        + grown * lane_sum(d_query_decayed * queries)
        - rest_hit
        + write * weighted_hit
    )
    d_cumul_row = jnp.sum(jnp.where(row == col, d_cumul, 0.0) - ratio_hit, axis=0, keepdims=True)
    at_end = jnp.sum(rest_hit, axis=0, keepdims=True) + total * jnp.sum(
        lane_sum(later * state), axis=0, keepdims=True
    )
    d_decay = lane_sum(jnp.where(col >= row, d_cumul_row, 0.0)) + at_end
    d_logit0 = d_decay * slope
    d_logit1 = d_write * write * (1.0 - write)

    d_queries = d_queries * SCALE
    grad_q = q_scale * (d_queries - q_unit * lane_sum(q_unit * d_queries))
    grad_k = k_scale * (d_keys - keys * lane_sum(keys * d_keys))
    grad_v = write * pulled
    low_qk = jnp.concatenate([grad_q, grad_k], 1).astype(jnp.bfloat16)
    low_v = grad_v.astype(jnp.bfloat16)

    fetch.wait()
    for peer in range(COLS):
        rows = pl.ds(peer * 2 * DK, 2 * DK)
        weights = jnp.concatenate([weight_ref[0, rows], weight_ref[1, rows]], 1)
        acc = lax.dot_general(low_qk, weights, NT, preferred_element_type=F32)
        acc = acc + lax.dot_general(low_v, weight_ref[2, rows], NT, preferred_element_type=F32)
        acc = acc + d_logit0 * gate_ref[0, :, rows].astype(F32)
        acc = acc + d_logit1 * gate_ref[1, :, rows].astype(F32)
        keep_ref[peer] = jnp.where(here_c == 0, acc[:, :DK], acc[:, DK:])
        send_ref[peer] = jnp.where(here_c == 0, acc[:, DK:], acc[:, :DK])


VMEM = pl.BlockSpec(memory_space=pltpu.VMEM)
SMEM = pl.BlockSpec(memory_space=pltpu.SMEM)
ANY = pl.BlockSpec(memory_space=pl.ANY)


def like(*shape):
    return jax.ShapeDtypeStruct(shape, F32)


def shards(projected, out_grad, logits, head_params, qkv_weight, gate_weight):
    chunks, saved = pl.pallas_call(
        chunk_kernel,
        out_shape=(like(COLS, DK + 2 * SLICE, DK), like(6, DK, DK)),
        in_specs=[VMEM, VMEM, VMEM, SMEM],
        out_specs=(VMEM, VMEM),
        name="chunk",
    )(projected, out_grad, logits, head_params)
    chunks = lax.all_to_all(chunks, "y", 0, 0, tiled=True)
    rows, own = pl.pallas_call(
        row_kernel,
        out_shape=(like(ROWS * COLS, 3 * SLICE, DK), like(2, DK, DK)),
        in_specs=[VMEM],
        out_specs=(VMEM, VMEM),
        scratch_shapes=[pltpu.VMEM((DK, DK), F32)],
        name="row",
    )(chunks)
    rows = lax.all_to_all(rows, ("x", "y"), 0, 0, tiled=True)
    keep, send = pl.pallas_call(
        grad_kernel,
        out_shape=(like(COLS, TOK, DK), like(COLS, TOK, DK)),
        in_specs=[VMEM, VMEM, VMEM, SMEM, ANY, VMEM, VMEM, VMEM, VMEM],
        out_specs=(VMEM, VMEM),
        scratch_shapes=[
            pltpu.VMEM((3, 2048, DK), jnp.bfloat16),
            pltpu.SemaphoreType.DMA(()),
        ],
        name="grad",
    )(projected, out_grad, logits, head_params, qkv_weight, gate_weight, saved, own, rows)
    other = lax.ppermute(send, "c", [(0, 1), (1, 0)])
    summed = lax.all_to_all(keep + other, "z", 0, 0, tiled=True)
    return summed.sum(axis=0).astype(jnp.bfloat16)


def solution(mesh):
    split = Mesh(mesh.devices.reshape(4, 8, 8, 2), ("x", "y", "z", "c"))
    seq, head = ("x", "y"), ("z", "c")
    in_specs = (
        P(None, seq, head),
        P(seq, head),
        P(None, head, seq),
        P(None, head),
        P(None, None, head),
        P(None, head, None),
    )
    return jax.shard_map(
        shards, mesh=split, in_specs=in_specs, out_specs=P(seq, head), check_vma=False
    )
```

```python
import jax
import jax.numpy as jnp
from jax import lax
from jax.experimental import pallas as pl
from jax.experimental.pallas import tpu as pltpu
from jax.sharding import Mesh
from jax.sharding import PartitionSpec as P

DK = 128
TOK = 128
ROWS = 4
COLS = 8
SLICE = DK // COLS
ORDER = (7, 5, 3, 6, 4, 2, 1, 0)
SCALE = DK ** (-0.5)
F32 = jnp.float32
CHUNK_LIMIT = 60 << 20

NN = (((1,), (0,)), ((), ()))
NT = (((1,), (1,)), ((), ()))
TN = (((0,), (0,)), ((), ()))


BF16 = jnp.bfloat16


def halves(x):
    if isinstance(x, tuple):
        return x
    high = x.astype(BF16)
    return high, (x - high.astype(F32)).astype(BF16)


def dot(left, right, dims=NN):
    (lh, ll), (rh, rl) = halves(left), halves(right)

    def one(a, b):
        return lax.dot_general(a, b, dims, preferred_element_type=F32)

    return one(lh, rh) + (one(lh, rl) + one(ll, rh))


def iotas():
    row = lax.broadcasted_iota(jnp.int32, (TOK, TOK), 0)
    col = lax.broadcasted_iota(jnp.int32, (TOK, TOK), 1)
    return row, col


def lane_sum(x):
    return jnp.sum(x, axis=1, keepdims=True)


def unit(raw):
    scale = lax.rsqrt(lane_sum(raw * raw) + 1.0)
    return raw * scale, scale


def gates(logit_ref, head_ref, row, col):
    heads = head_ref[...]
    rate = jnp.exp(heads[:, 0:1])
    shifted = logit_ref[0] + heads[:, 1:2]
    soft = jnp.maximum(shifted, 0.0) + jnp.log1p(jnp.exp(-jnp.abs(shifted)))
    decay_row = -rate * soft
    cumul = lane_sum(jnp.where(col <= row, decay_row, 0.0))
    cumul_row = jnp.sum(jnp.where(row == col, cumul, 0.0), axis=0, keepdims=True)
    last = cumul_row[:, TOK - 1 :]
    write = lane_sum(jnp.where(row == col, jax.nn.sigmoid(logit_ref[1]), 0.0))
    lower = row >= col
    ratio = jnp.where(lower, jnp.exp(jnp.where(lower, cumul - cumul_row, 0.0)), 0.0)
    slope = lane_sum(jnp.where(row == col, -rate * jax.nn.sigmoid(shifted), 0.0))
    return jnp.exp(cumul), jnp.exp(last - cumul), jnp.exp(last), write, ratio, slope


def inverse_of(strict, row, col):
    eye = jnp.where(row == col, 1.0, 0.0).astype(F32)
    near = jnp.where((row >> 3) == (col >> 3), strict, 0.0)
    power2 = dot(near, near)
    out = eye - near
    both = dot(jnp.concatenate([out, power2], 0), power2)
    out, power4 = out + both[:TOK], both[TOK:]
    out = out + dot(out, power4)
    for level in (3, 4, 5, 6):
        joined = ((row >> (level + 1)) == (col >> (level + 1))) & ((row >> level) != (col >> level))
        off = jnp.where(joined, strict, 0.0)
        pair = halves(out)
        out = out - dot(pair, dot(off, pair))
    return out


def chunk_kernel(
    proj_hbm,
    grad_hbm,
    logit_hbm,
    head_hbm,
    out_ref,
    saved_ref,
    proj_ref,
    grad_ref,
    logit_ref,
    head_ref,
    sems,
):
    pairs = (
        (logit_hbm, logit_ref),
        (head_hbm, head_ref),
        (proj_hbm, proj_ref),
        (grad_hbm, grad_ref),
    )
    copies = [pltpu.make_async_copy(*pair, sems.at[i]) for i, pair in enumerate(pairs)]
    for copy in copies:
        copy.start()
    for copy in copies:
        copy.wait()
    row, col = iotas()
    grown, rest, total, write, ratio, _ = gates(logit_ref, head_ref, row, col)
    queries = unit(proj_ref[0].astype(F32))[0] * SCALE
    keys = unit(proj_ref[1].astype(F32))[0]
    values = proj_ref[2].astype(F32)
    out_grad = grad_ref[...].astype(F32)
    inner = dot(jnp.concatenate([keys, queries], 0), keys, NT)
    bare = jnp.where(row > col, ratio * inner[:TOK], 0.0)
    attend = ratio * inner[TOK:]
    inverse = inverse_of(bare * write, row, col)
    solved = dot(inverse, jnp.concatenate([(write * grown) * keys, write * values], 1))
    key_weights, base = solved[:, :DK], solved[:, DK:]
    rest_keys = rest * keys
    moved = dot(solved, rest_keys, TN)
    eye = jnp.where(row == col, 1.0, 0.0).astype(F32)
    step = total * eye - moved[:DK]
    offset = moved[DK:]
    back = dot(out_grad, grown * queries - dot(attend, key_weights), TN)
    for peer in range(COLS):
        out_ref[peer, :DK] = step
        out_ref[peer, DK : DK + SLICE] = offset[peer * SLICE : (peer + 1) * SLICE]
        out_ref[peer, DK + SLICE :] = back[peer * SLICE : (peer + 1) * SLICE]
    saved_ref[0] = inverse.T
    saved_ref[1] = key_weights
    saved_ref[2] = base
    saved_ref[3] = attend
    saved_ref[4] = bare
    saved_ref[5] = dot(attend, out_grad, TN)


def row_kernel(in_ref, out_ref, own_ref, scratch_ref):
    here_x = lax.axis_index("x")
    here_y = lax.axis_index("y")
    step = [in_ref[j, :DK] for j in range(COLS)]
    ahead = [in_ref[j, DK : DK + SLICE] for j in range(COLS)]
    back = [in_ref[j, DK + SLICE :] for j in range(COLS)]

    def joined(first, second):
        both = dot(jnp.concatenate([first[0], first[1]], 0), second[0])
        return (both[:DK], both[DK:] + second[1], first[2] + dot(second[2], first[0], NT))

    ones = list(zip(step, ahead, back))
    pairs = [joined(ones[2 * i], ones[2 * i + 1]) for i in range(4)]
    quads = [joined(pairs[2 * i], pairs[2 * i + 1]) for i in range(2)]
    whole = joined(quads[0], quads[1])

    zero = jnp.zeros((SLICE, DK), F32)
    b4 = quads[0][1]
    b2 = pairs[0][1]
    b6 = dot(b4, pairs[2][0]) + pairs[2][1]
    prefix = [
        zero,
        ahead[0],
        b2,
        dot(b2, step[2]) + ahead[2],
        b4,
        dot(b4, step[4]) + ahead[4],
        b6,
        dot(b6, step[6]) + ahead[6],
    ]
    c3 = quads[1][2]
    c5 = pairs[3][2]
    c1 = dot(c3, pairs[1][0], NT) + pairs[1][2]
    suffix = [
        dot(c1, step[1], NT) + back[1],
        c1,
        dot(c3, step[3], NT) + back[3],
        c3,
        dot(c5, step[5], NT) + back[5],
        c5,
        back[7],
        zero,
    ]

    row, col = iotas()
    eye = jnp.where(row == col, 1.0, 0.0).astype(F32)
    at_y = jnp.full((DK, DK), here_y, jnp.int32)
    high = at_y >= 4
    mid = (at_y & 2) != 0
    low = (at_y & 1) != 0
    before = jnp.where(high, quads[0][0], eye)
    before = dot(before, jnp.where(mid, jnp.where(high, pairs[2][0], pairs[0][0]), eye))
    single = in_ref[jnp.maximum(here_y - 1, 0), :DK]
    own_ref[0] = dot(before, jnp.where(low, single, eye))
    after = jnp.where(high, eye, quads[1][0])
    after = dot(jnp.where(mid, eye, jnp.where(high, pairs[3][0], pairs[1][0])), after)
    single = in_ref[jnp.minimum(here_y + 1, COLS - 1), :DK]
    own_ref[1] = dot(jnp.where(low, eye, single), after)

    scratch_ref[...] = whole[0]
    piece = scratch_ref[pl.ds(pl.multiple_of(here_y * SLICE, SLICE), SLICE)]
    at_x = jnp.full((SLICE, DK), here_x, jnp.int32)
    for peer_x in range(ROWS):
        own = at_x == peer_x
        sent = jnp.where(at_x < peer_x, whole[1], whole[2])
        for peer_y in range(COLS):
            slot = peer_x * COLS + peer_y
            out_ref[slot, :SLICE] = jnp.where(own, prefix[peer_y], piece)
            out_ref[slot, SLICE:] = jnp.where(own, suffix[peer_y], sent)


def grad_kernel(
    proj_ref,
    grad_ref,
    logit_ref,
    head_ref,
    weight_ref,
    gate_ref,
    saved_ref,
    own_ref,
    in_ref,
    send_ref,
    low_ref,
    slope_ref,
):
    here_x = lax.axis_index("x")
    here_c = lax.axis_index("c")

    def part(row_at, kind):
        rows = pl.ds(row_at * COLS, COLS)
        return in_ref[rows, kind * SLICE : (kind + 1) * SLICE].reshape(DK, DK)

    step1, step2 = halves(part(1, 0)), halves(part(2, 0))
    s1 = part(0, 1)
    s2 = dot(s1, step1) + part(1, 1)
    s3 = dot(s2, step2) + part(2, 1)
    g2 = part(3, 1)
    g1 = dot(g2, step2, NT) + part(2, 1)
    g0 = dot(g1, step1, NT) + part(1, 1)
    zero = jnp.zeros((DK, DK), F32)
    s_row = jnp.where(here_x == 0, zero, jnp.where(here_x == 1, s1, jnp.where(here_x == 2, s2, s3)))
    g_row = jnp.where(here_x == 3, zero, jnp.where(here_x == 2, g2, jnp.where(here_x == 1, g1, g0)))
    state = dot(s_row, own_ref[0]) + part(here_x, 0)
    later = dot(g_row, own_ref[1], NT) + part(here_x, 1)

    row, col = iotas()
    grown, rest, total, write, ratio, slope = gates(logit_ref, head_ref, row, col)
    q_unit, q_scale = unit(proj_ref[0].astype(F32))
    queries = q_unit * SCALE
    keys, k_scale = unit(proj_ref[1].astype(F32))
    values = proj_ref[2].astype(F32)
    out_grad = grad_ref[...].astype(F32)
    rest_keys = rest * keys
    attend = saved_ref[3]
    bare = saved_ref[4]

    fresh = saved_ref[2] - dot(saved_ref[1], state, NT)
    d_fresh = saved_ref[5] + dot(rest_keys, later, NT)
    pulled = dot(saved_ref[0], d_fresh)
    both = dot(jnp.concatenate([out_grad, pulled], 0), state)
    d_query_decayed = both[:TOK]
    d_weighted = -both[TOK:]
    d_rest = dot(fresh, later)
    both = dot(jnp.concatenate([out_grad, pulled], 0), fresh, NT)
    d_attend = jnp.where(row >= col, both[:TOK], 0.0)
    d_lower = jnp.where(row > col, -both[TOK:], 0.0)
    d_qk = d_attend * ratio
    d_kk = d_lower * ratio * write
    stacked = jnp.concatenate([d_qk, d_kk], 0)
    by_key = dot(stacked, keys)
    across = dot(stacked, jnp.concatenate([queries, keys], 0), TN)
    d_queries = grown * d_query_decayed + by_key[:TOK]
    d_keys = by_key[TOK:] + across + rest * d_rest + (write * grown) * d_weighted

    lower_hit = d_lower * bare
    ratio_hit = d_attend * attend + lower_hit * write
    weighted_hit = grown * lane_sum(d_weighted * keys)
    rest_hit = lane_sum(d_rest * rest_keys)
    d_write = lane_sum(pulled * values) + weighted_hit + lane_sum(lower_hit)
    d_cumul = (
        lane_sum(ratio_hit)
        + grown * lane_sum(d_query_decayed * queries)
        - rest_hit
        + write * weighted_hit
    )
    d_cumul_row = jnp.sum(jnp.where(row == col, d_cumul, 0.0) - ratio_hit, axis=0, keepdims=True)
    at_end = jnp.sum(rest_hit, axis=0, keepdims=True) + total * jnp.sum(
        lane_sum(later * state), axis=0, keepdims=True
    )
    d_decay = lane_sum(jnp.where(col >= row, d_cumul_row, 0.0)) + at_end
    d_logit0 = d_decay * slope
    d_logit1 = d_write * write * (1.0 - write)

    d_queries = d_queries * SCALE
    grad_q = q_scale * (d_queries - q_unit * lane_sum(q_unit * d_queries))
    grad_k = k_scale * (d_keys - keys * lane_sum(keys * d_keys))
    grad_v = write * pulled
    low = [grad.astype(BF16) for grad in (grad_q, grad_k, grad_v)]
    for source in range(3):
        low_ref[source] = low[source]
    slopes = (d_logit0, d_logit1)
    slope_ref[...] = jnp.where(col == 0, d_logit0, d_logit1)
    for slot, peer in enumerate(ORDER):
        send_ref[slot] = projected_to(2 * peer + 1 - here_c, low, slopes, weight_ref, gate_ref)


def projected_to(head, low, slopes, weight_ref, gate_ref):
    at = pl.multiple_of(head * DK, DK)
    rows = pl.ds(at, DK)
    weights = jnp.concatenate([weight_ref[0, rows], weight_ref[1, rows]], 1)
    acc = lax.dot_general(
        jnp.concatenate(low[:2], 1), weights, NT, preferred_element_type=F32
    ) + lax.dot_general(low[2], weight_ref[2, rows], NT, preferred_element_type=F32)
    for kind in range(2):
        acc = acc + slopes[kind] * gate_ref[kind : kind + 1, rows].astype(F32)
    return acc


def keep_kernel(low_ref, slope_ref, weight_ref, gate_ref, other_ref, out_ref):
    here_c = lax.axis_index("c")
    low = [low_ref[source] for source in range(3)]
    slopes = (slope_ref[:, 0:1], slope_ref[:, 1:2])
    for slot, peer in enumerate(ORDER):
        own = projected_to(2 * peer + here_c, low, slopes, weight_ref, gate_ref)
        out_ref[slot] = other_ref[slot] + own


VMEM = pl.BlockSpec(memory_space=pltpu.VMEM)
HBM = pl.BlockSpec(memory_space=pltpu.HBM)


def like(*shape):
    return jax.ShapeDtypeStruct(shape, F32)


def call(kernel, name, out_shape, in_specs, *args, scratch=(), limit=16 << 20):
    return pl.pallas_call(
        kernel,
        out_shape=out_shape,
        in_specs=in_specs,
        out_specs=jax.tree.map(lambda _: VMEM, out_shape),
        scratch_shapes=scratch,
        compiler_params=pltpu.CompilerParams(vmem_limit_bytes=limit),
        name=name,
    )(*args)


def shards(projected, out_grad, logits, head_params, qkv_weight, gate_weight):
    heads = head_params.T
    gate = jnp.transpose(gate_weight, (1, 0, 2))[0]
    chunks, saved = call(
        chunk_kernel,
        "chunk",
        (like(COLS, DK + 2 * SLICE, DK), like(6, DK, DK)),
        [HBM] * 4,
        projected,
        out_grad,
        logits,
        heads,
        scratch=[
            pltpu.VMEM((3, TOK, DK), BF16),
            pltpu.VMEM((TOK, DK), BF16),
            pltpu.VMEM((2, 1, TOK), F32),
            pltpu.VMEM((1, 2), F32),
            pltpu.SemaphoreType.DMA((4,)),
        ],
        limit=CHUNK_LIMIT,
    )
    chunks = lax.all_to_all(chunks, "y", 0, 0, tiled=True)
    rows, own = call(
        row_kernel,
        "row",
        (like(ROWS * COLS, 2 * SLICE, DK), like(2, DK, DK)),
        [VMEM],
        chunks,
        scratch=[pltpu.VMEM((DK, DK), F32)],
    )
    rows = lax.all_to_all(rows, ("x", "y"), 0, 0, tiled=True)
    send, low, slopes = call(
        grad_kernel,
        "grad",
        (
            like(COLS, TOK, DK),
            jax.ShapeDtypeStruct((3, TOK, DK), BF16),
            like(TOK, DK),
        ),
        [VMEM] * 9,
        projected,
        out_grad,
        logits,
        heads,
        qkv_weight,
        gate,
        saved,
        own,
        rows,
    )
    other = lax.ppermute(send, "c", [(0, 1), (1, 0)])
    part = call(
        keep_kernel,
        "keep",
        like(COLS, TOK, DK),
        [VMEM] * 5,
        low,
        slopes,
        qkv_weight,
        gate,
        other,
    )
    summed = lax.all_to_all(
        part, "z", 0, 0, tiled=True, axis_index_groups=[list(ORDER)]
    )
    return summed.sum(axis=0).astype(BF16)


def solution(mesh):
    split = Mesh(mesh.devices.reshape(4, 8, 8, 2), ("x", "y", "z", "c"))
    seq, head = ("x", "y"), ("z", "c")
    in_specs = (
        P(None, seq, head),
        P(seq, head),
        P(None, head, seq),
        P(None, head),
        P(None, None, head),
        P(None, head, None),
    )
    return jax.shard_map(
        shards, mesh=split, in_specs=in_specs, out_specs=P(seq, head), check_vma=False
    )
```

```python
import jax
import jax.numpy as jnp
from jax import lax
from jax.experimental import pallas as pl
from jax.experimental.pallas import tpu as pltpu
from jax.sharding import Mesh
from jax.sharding import PartitionSpec as P

DK = 128
TOK = 128
ROWS = 4
COLS = 8
SLICE = DK // COLS
ORDER = (7, 5, 3, 6, 4, 2, 1, 0)
GRID_ORDER = tuple(x * COLS + y for y in reversed(range(COLS)) for x in range(ROWS))
SCALE = DK ** (-0.5)
F32 = jnp.float32
CHUNK_LIMIT = 60 << 20

NN = (((1,), (0,)), ((), ()))
NT = (((1,), (1,)), ((), ()))
TN = (((0,), (0,)), ((), ()))


BF16 = jnp.bfloat16


def halves(x):
    if isinstance(x, tuple):
        return x
    high = x.astype(BF16)
    return high, (x - high.astype(F32)).astype(BF16)


def whole(pair):
    return pair[0].astype(F32) + pair[1].astype(F32)


def dot(left, right, dims=NN):
    (lh, ll), (rh, rl) = halves(left), halves(right)
    (lk,), (rk,) = dims[0]
    both = jnp.concatenate([lh, ll], lk)
    if rh.shape[1 - rk] == DK:
        first = jnp.concatenate([rh, rh], rk)
        second = jnp.concatenate([rl, jnp.zeros_like(rl)], rk)
        out = lax.dot_general(
            both, jnp.concatenate([first, second], 1 - rk), dims, preferred_element_type=F32
        )
        return out[:, :DK] + out[:, DK:]
    out = lax.dot_general(both, jnp.concatenate([rh, rh], rk), dims, preferred_element_type=F32)
    return out + lax.dot_general(lh, rl, dims, preferred_element_type=F32)


def iotas():
    row = lax.broadcasted_iota(jnp.int32, (TOK, TOK), 0)
    col = lax.broadcasted_iota(jnp.int32, (TOK, TOK), 1)
    return row, col


def lane_sum(x):
    return jnp.sum(x, axis=1, keepdims=True)


def unit(raw):
    scale = lax.rsqrt(lane_sum(raw * raw) + 1.0)
    return raw * scale, scale


def gates(logit_ref, head_ref, row, col):
    heads = head_ref[...]
    rate = jnp.exp(heads[:, 0:1])
    shifted = logit_ref[0] + heads[:, 1:2]
    soft = jnp.maximum(shifted, 0.0) + jnp.log1p(jnp.exp(-jnp.abs(shifted)))
    decay_row = -rate * soft
    cumul = lane_sum(jnp.where(col <= row, decay_row, 0.0))
    cumul_row = jnp.sum(jnp.where(row == col, cumul, 0.0), axis=0, keepdims=True)
    last = cumul_row[:, TOK - 1 :]
    write = lane_sum(jnp.where(row == col, jax.nn.sigmoid(logit_ref[1]), 0.0))
    lower = row >= col
    ratio = jnp.where(lower, jnp.exp(jnp.where(lower, cumul - cumul_row, 0.0)), 0.0)
    slope = lane_sum(jnp.where(row == col, -rate * jax.nn.sigmoid(shifted), 0.0))
    return jnp.exp(cumul), jnp.exp(last - cumul), jnp.exp(last), write, ratio, slope


def inverse_of(strict, row, col):
    eye = jnp.where(row == col, 1.0, 0.0).astype(F32)

    def same(level):
        return (row >> level) == (col >> level)

    out = eye - jnp.where(same(1), strict, 0.0)
    for low, high in ((1, 4), (4, 7)):
        near = halves(out)
        off = jnp.where(same(high) & ~same(low), strict, 0.0)
        power = dot(near, off)
        both = dot(power, jnp.concatenate([power, out], 1))
        power, out = both[:, :TOK], out - both[:, TOK:]
        both = dot(power, jnp.concatenate([power, out], 1))
        power, out = both[:, :TOK], out + both[:, TOK:]
        out = out + dot(power, out)
    return out


def chunk_kernel(
    proj_hbm,
    grad_hbm,
    logit_hbm,
    head_hbm,
    out_hbm,
    saved_hbm,
    proj_ref,
    grad_ref,
    logit_ref,
    head_ref,
    step_ref,
    edge_ref,
    saved_ref,
    in_sems,
    out_sems,
):
    pairs = (
        (logit_hbm, logit_ref),
        (head_hbm, head_ref),
        (proj_hbm, proj_ref),
        (grad_hbm, grad_ref),
    )
    copies = [pltpu.make_async_copy(*pair, in_sems.at[i]) for i, pair in enumerate(pairs)]
    for copy in copies:
        copy.start()
    for copy in copies:
        copy.wait()
    leaving = []

    def leave(source, target):
        copy = pltpu.make_async_copy(source, target, out_sems.at[len(leaving)])
        copy.start()
        leaving.append(copy)

    def save(at, value):
        saved_ref[at] = value
        leave(saved_ref.at[at], saved_hbm.at[at])

    row, col = iotas()
    grown, rest, total, write, ratio, _ = gates(logit_ref, head_ref, row, col)
    queries = unit(proj_ref[0].astype(F32))[0] * SCALE
    keys = unit(proj_ref[1].astype(F32))[0]
    values = proj_ref[2].astype(F32)
    out_grad = grad_ref[...].astype(F32)
    inner = dot(jnp.concatenate([keys, queries], 0), keys, NT)
    bare = jnp.where(row > col, ratio * inner[:TOK], 0.0)
    attend = ratio * inner[TOK:]
    inverse = inverse_of(bare * write, row, col)
    attended = dot(attend, out_grad, TN)
    direct = dot(out_grad, grown * queries, TN)
    solved = dot(inverse, jnp.concatenate([(write * grown) * keys, write * values], 1))
    key_weights, base = solved[:, :DK], solved[:, DK:]
    rest_keys = rest * keys
    moved = dot(solved, rest_keys, TN)
    eye = jnp.where(row == col, 1.0, 0.0).astype(F32)
    step_ref[...] = total * eye - moved[:DK]
    for peer in range(COLS):
        leave(step_ref, out_hbm.at[peer, pl.ds(0, DK)])
    back = direct - dot(attended, key_weights, TN)
    for peer in range(COLS):
        edge_ref[peer, :SLICE] = moved[DK + peer * SLICE : DK + (peer + 1) * SLICE]
        edge_ref[peer, SLICE:] = back[peer * SLICE : (peer + 1) * SLICE]
    leave(edge_ref, out_hbm.at[:, pl.ds(DK, 2 * SLICE)])
    save(0, inverse.T)
    save(1, key_weights)
    save(2, base)
    save(3, attend)
    save(4, bare)
    save(5, attended)
    for copy in leaving:
        copy.wait()


def row_kernel(in_ref, out_ref, own_ref, scratch_ref):
    here_x = lax.axis_index("x")
    here_y = lax.axis_index("y")
    step = [in_ref[j, :DK] for j in range(COLS)]
    ahead = [in_ref[j, DK : DK + SLICE] for j in range(COLS)]
    back = [in_ref[j, DK + SLICE :] for j in range(COLS)]

    def joined(first, second):
        both = dot(jnp.concatenate([first[0], first[1]], 0), second[0])
        return (both[:DK], both[DK:] + second[1], first[2] + dot(second[2], first[0], NT))

    ones = list(zip(step, ahead, back))
    pairs = [joined(ones[2 * i], ones[2 * i + 1]) for i in range(4)]
    quads = [joined(pairs[2 * i], pairs[2 * i + 1]) for i in range(2)]
    whole = joined(quads[0], quads[1])

    zero = jnp.zeros((SLICE, DK), F32)
    b4 = quads[0][1]
    b2 = pairs[0][1]
    b6 = dot(b4, pairs[2][0]) + pairs[2][1]
    prefix = [
        zero,
        ahead[0],
        b2,
        dot(b2, step[2]) + ahead[2],
        b4,
        dot(b4, step[4]) + ahead[4],
        b6,
        dot(b6, step[6]) + ahead[6],
    ]
    c3 = quads[1][2]
    c5 = pairs[3][2]
    c1 = dot(c3, pairs[1][0], NT) + pairs[1][2]
    suffix = [
        dot(c1, step[1], NT) + back[1],
        c1,
        dot(c3, step[3], NT) + back[3],
        c3,
        dot(c5, step[5], NT) + back[5],
        c5,
        back[7],
        zero,
    ]

    row, col = iotas()
    eye = jnp.where(row == col, 1.0, 0.0).astype(F32)
    at_y = jnp.full((DK, DK), here_y, jnp.int32)
    high = at_y >= 4
    mid = (at_y & 2) != 0
    low = (at_y & 1) != 0
    before = jnp.where(high, quads[0][0], eye)
    before = dot(before, jnp.where(mid, jnp.where(high, pairs[2][0], pairs[0][0]), eye))
    single = in_ref[jnp.maximum(here_y - 1, 0), :DK]
    own_ref[0] = dot(before, jnp.where(low, single, eye))
    after = jnp.where(high, eye, quads[1][0])
    after = dot(jnp.where(mid, eye, jnp.where(high, pairs[3][0], pairs[1][0])), after)
    single = in_ref[jnp.minimum(here_y + 1, COLS - 1), :DK]
    own_ref[1] = dot(jnp.where(low, eye, single), after)

    scratch_ref[...] = whole[0]
    piece = scratch_ref[pl.ds(pl.multiple_of(here_y * SLICE, SLICE), SLICE)]
    at_x = jnp.full((SLICE, DK), here_x, jnp.int32)
    for peer_x in range(ROWS):
        own = at_x == peer_x
        sent = jnp.where(at_x < peer_x, whole[1], whole[2])
        for peer_y in range(COLS):
            slot = (COLS - 1 - peer_y) * ROWS + peer_x
            out_ref[slot, :SLICE] = jnp.where(own, prefix[peer_y], piece)
            out_ref[slot, SLICE:] = jnp.where(own, suffix[peer_y], sent)


def grad_kernel(
    proj_ref,
    grad_ref,
    logit_ref,
    head_ref,
    weight_ref,
    gate_ref,
    saved_ref,
    own_ref,
    in_ref,
    send_ref,
    low_ref,
    slope_ref,
):
    here_x = lax.axis_index("x")
    here_c = lax.axis_index("c")

    def part(row_at, kind):
        span = slice(kind * SLICE, (kind + 1) * SLICE)
        slots = [(COLS - 1 - y) * ROWS + row_at for y in range(COLS)]
        return jnp.concatenate([in_ref[slot, span] for slot in slots], 0)

    step1, step2 = halves(part(1, 0)), halves(part(2, 0))
    s1 = part(0, 1)
    s2 = dot(s1, step1) + part(1, 1)
    s3 = dot(s2, step2) + part(2, 1)
    g2 = part(3, 1)
    g1 = dot(g2, step2, NT) + part(2, 1)
    g0 = dot(g1, step1, NT) + part(1, 1)
    zero = jnp.zeros((DK, DK), F32)
    s_row = jnp.where(here_x == 0, zero, jnp.where(here_x == 1, s1, jnp.where(here_x == 2, s2, s3)))
    g_row = jnp.where(here_x == 3, zero, jnp.where(here_x == 2, g2, jnp.where(here_x == 1, g1, g0)))
    state = halves(dot(s_row, own_ref[0]) + part(here_x, 0))
    later = halves(dot(g_row, own_ref[1], NT) + part(here_x, 1))

    row, col = iotas()
    grown, rest, total, write, ratio, slope = gates(logit_ref, head_ref, row, col)
    q_unit, q_scale = unit(proj_ref[0].astype(F32))
    queries = q_unit * SCALE
    keys, k_scale = unit(proj_ref[1].astype(F32))
    values = proj_ref[2].astype(F32)
    out_grad = grad_ref[...].astype(F32)
    rest_keys = rest * keys
    attend = saved_ref[3]
    bare = saved_ref[4]

    fresh = halves(saved_ref[2] - dot(saved_ref[1], state, NT))
    d_fresh = saved_ref[5] + dot(rest_keys, later, NT)
    pulled = dot(saved_ref[0], d_fresh)
    both = dot(jnp.concatenate([out_grad, pulled], 0), state)
    d_query_decayed = both[:TOK]
    d_weighted = -both[TOK:]
    d_rest = dot(fresh, later)
    both = dot(jnp.concatenate([out_grad, pulled], 0), fresh, NT)
    d_attend = jnp.where(row >= col, both[:TOK], 0.0)
    d_lower = jnp.where(row > col, -both[TOK:], 0.0)
    d_qk = d_attend * ratio
    d_kk = d_lower * ratio * write
    stacked = jnp.concatenate([d_qk, d_kk], 0)
    by_key = dot(stacked, keys)
    across = dot(stacked, jnp.concatenate([queries, keys], 0), TN)
    d_queries = grown * d_query_decayed + by_key[:TOK]
    d_keys = by_key[TOK:] + across + rest * d_rest + (write * grown) * d_weighted

    lower_hit = d_lower * bare
    ratio_hit = d_attend * attend + lower_hit * write
    weighted_hit = grown * lane_sum(d_weighted * keys)
    rest_hit = lane_sum(d_rest * rest_keys)
    d_write = lane_sum(pulled * values) + weighted_hit + lane_sum(lower_hit)
    d_cumul = (
        lane_sum(ratio_hit)
        + grown * lane_sum(d_query_decayed * queries)
        - rest_hit
        + write * weighted_hit
    )
    d_cumul_row = jnp.sum(jnp.where(row == col, d_cumul, 0.0) - ratio_hit, axis=0, keepdims=True)
    at_end = jnp.sum(rest_hit, axis=0, keepdims=True) + total * jnp.sum(
        lane_sum(whole(later) * whole(state)), axis=0, keepdims=True
    )
    d_decay = lane_sum(jnp.where(col >= row, d_cumul_row, 0.0)) + at_end
    d_logit0 = d_decay * slope
    d_logit1 = d_write * write * (1.0 - write)

    d_queries = d_queries * SCALE
    grad_q = q_scale * (d_queries - q_unit * lane_sum(q_unit * d_queries))
    grad_k = k_scale * (d_keys - keys * lane_sum(keys * d_keys))
    grad_v = write * pulled
    low = [grad.astype(BF16) for grad in (grad_q, grad_k, grad_v)]
    for source in range(3):
        low_ref[source] = low[source]
    slopes = (d_logit0, d_logit1)
    slope_ref[...] = jnp.where(col == 0, d_logit0, d_logit1)
    for slot, peer in enumerate(ORDER):
        send_ref[slot] = projected_to(2 * peer + 1 - here_c, low, slopes, weight_ref, gate_ref)


def projected_to(head, low, slopes, weight_ref, gate_ref):
    at = pl.multiple_of(head * DK, DK)
    rows = pl.ds(at, DK)
    weights = jnp.concatenate([weight_ref[0, rows], weight_ref[1, rows]], 1)
    acc = lax.dot_general(
        jnp.concatenate(low[:2], 1), weights, NT, preferred_element_type=F32
    ) + lax.dot_general(low[2], weight_ref[2, rows], NT, preferred_element_type=F32)
    for kind in range(2):
        acc = acc + slopes[kind] * gate_ref[kind : kind + 1, rows].astype(F32)
    return acc


def keep_kernel(low_ref, slope_ref, weight_ref, gate_ref, other_ref, out_ref):
    here_c = lax.axis_index("c")
    low = [low_ref[source] for source in range(3)]
    slopes = (slope_ref[:, 0:1], slope_ref[:, 1:2])
    for slot, peer in enumerate(ORDER):
        own = projected_to(2 * peer + here_c, low, slopes, weight_ref, gate_ref)
        out_ref[slot] = other_ref[slot] + own


VMEM = pl.BlockSpec(memory_space=pltpu.VMEM)
HBM = pl.BlockSpec(memory_space=pltpu.HBM)


def like(*shape):
    return jax.ShapeDtypeStruct(shape, F32)


def call(kernel, name, out_shape, in_specs, *args, scratch=(), limit=16 << 20, space=VMEM):
    return pl.pallas_call(
        kernel,
        out_shape=out_shape,
        in_specs=in_specs,
        out_specs=jax.tree.map(lambda _: space, out_shape),
        scratch_shapes=scratch,
        compiler_params=pltpu.CompilerParams(vmem_limit_bytes=limit),
        name=name,
    )(*args)


def shards(projected, out_grad, logits, head_params, qkv_weight, gate_weight):
    heads = head_params.T
    gate = jnp.transpose(gate_weight, (1, 0, 2))[0]
    chunks, saved = call(
        chunk_kernel,
        "chunk",
        (like(COLS, DK + 2 * SLICE, DK), like(6, DK, DK)),
        [HBM] * 4,
        projected,
        out_grad,
        logits,
        heads,
        scratch=[
            pltpu.VMEM((3, TOK, DK), BF16),
            pltpu.VMEM((TOK, DK), BF16),
            pltpu.VMEM((2, 1, TOK), F32),
            pltpu.VMEM((1, 2), F32),
            pltpu.VMEM((DK, DK), F32),
            pltpu.VMEM((COLS, 2 * SLICE, DK), F32),
            pltpu.VMEM((6, DK, DK), F32),
            pltpu.SemaphoreType.DMA((4,)),
            pltpu.SemaphoreType.DMA((COLS + 7,)),
        ],
        space=HBM,
        limit=CHUNK_LIMIT,
    )
    chunks = lax.all_to_all(chunks, "y", 0, 0, tiled=True)
    rows, own = call(
        row_kernel,
        "row",
        (like(ROWS * COLS, 2 * SLICE, DK), like(2, DK, DK)),
        [VMEM],
        chunks,
        scratch=[pltpu.VMEM((DK, DK), F32)],
    )
    rows = lax.all_to_all(
        rows, ("x", "y"), 0, 0, tiled=True, axis_index_groups=[list(GRID_ORDER)]
    )
    send, low, slopes = call(
        grad_kernel,
        "grad",
        (
            like(COLS, TOK, DK),
            jax.ShapeDtypeStruct((3, TOK, DK), BF16),
            like(TOK, DK),
        ),
        [VMEM] * 9,
        projected,
        out_grad,
        logits,
        heads,
        qkv_weight,
        gate,
        saved,
        own,
        rows,
    )
    other = lax.ppermute(send, "c", [(0, 1), (1, 0)])
    part = call(
        keep_kernel,
        "keep",
        like(COLS, TOK, DK),
        [VMEM] * 5,
        low,
        slopes,
        qkv_weight,
        gate,
        other,
    )
    summed = lax.all_to_all(
        part, "z", 0, 0, tiled=True, axis_index_groups=[list(ORDER)]
    )
    return summed.sum(axis=0).astype(BF16)


def solution(mesh):
    split = Mesh(mesh.devices.reshape(4, 8, 8, 2), ("x", "y", "z", "c"))
    seq, head = ("x", "y"), ("z", "c")
    in_specs = (
        P(None, seq, head),
        P(seq, head),
        P(None, head, seq),
        P(None, head),
        P(None, None, head),
        P(None, head, None),
    )
    return jax.shard_map(
        shards, mesh=split, in_specs=in_specs, out_specs=P(seq, head), check_vma=False
    )
```

```python
import jax
import jax.numpy as jnp
from jax import lax
from jax.experimental import pallas as pl
from jax.experimental.pallas import tpu as pltpu
from jax.sharding import Mesh
from jax.sharding import PartitionSpec as P

DK = 128
TOK = 128
ROWS = 4
COLS = 8
SLICE = DK // COLS
ORDER = (7, 5, 3, 6, 4, 2, 1, 0)
GRID_ORDER = tuple(x * COLS + y for y in reversed(range(COLS)) for x in range(ROWS))
SCALE = DK ** (-0.5)
F32 = jnp.float32

NN = (((1,), (0,)), ((), ()))
NT = (((1,), (1,)), ((), ()))
TN = (((0,), (0,)), ((), ()))


BF16 = jnp.bfloat16


def halves(x):
    if isinstance(x, tuple):
        return x
    high = x.astype(BF16)
    return high, (x - high.astype(F32)).astype(BF16)


def whole(pair):
    return pair[0].astype(F32) + pair[1].astype(F32)


def dot(left, right, dims=NN):
    (lh, ll), (rh, rl) = halves(left), halves(right)
    (lk,), (rk,) = dims[0]
    both = jnp.concatenate([lh, ll], lk)
    if rh.shape[1 - rk] == DK:
        first = jnp.concatenate([rh, rh], rk)
        second = jnp.concatenate([rl, jnp.zeros_like(rl)], rk)
        out = lax.dot_general(
            both, jnp.concatenate([first, second], 1 - rk), dims, preferred_element_type=F32
        )
        return out[:, :DK] + out[:, DK:]
    out = lax.dot_general(both, jnp.concatenate([rh, rh], rk), dims, preferred_element_type=F32)
    return out + lax.dot_general(lh, rl, dims, preferred_element_type=F32)


def iotas():
    row = lax.broadcasted_iota(jnp.int32, (TOK, TOK), 0)
    col = lax.broadcasted_iota(jnp.int32, (TOK, TOK), 1)
    return row, col


def lane_sum(x):
    return jnp.sum(x, axis=1, keepdims=True)


def unit(raw):
    scale = lax.rsqrt(lane_sum(raw * raw) + 1.0)
    return raw * scale, scale


def gates(gate_rows_ref, row, col):
    rows = gate_rows_ref[...]
    rate = jnp.exp(rows[2:3, 0:1])
    shifted = rows[0:1] + rows[2:3, 1:2]
    soft = jnp.maximum(shifted, 0.0) + jnp.log1p(jnp.exp(-jnp.abs(shifted)))
    decay_row = -rate * soft
    cumul = lane_sum(jnp.where(col <= row, decay_row, 0.0))
    cumul_row = jnp.sum(jnp.where(row == col, cumul, 0.0), axis=0, keepdims=True)
    last = cumul_row[:, TOK - 1 :]
    write = lane_sum(jnp.where(row == col, jax.nn.sigmoid(rows[1:2]), 0.0))
    lower = row >= col
    ratio = jnp.where(lower, jnp.exp(jnp.where(lower, cumul - cumul_row, 0.0)), 0.0)
    slope = lane_sum(jnp.where(row == col, -rate * jax.nn.sigmoid(shifted), 0.0))
    return jnp.exp(cumul), jnp.exp(last - cumul), jnp.exp(last), write, ratio, slope


def inverse_of(strict, row, col):
    eye = jnp.where(row == col, 1.0, 0.0).astype(F32)

    def same(level):
        return (row >> level) == (col >> level)

    out = eye - jnp.where(same(1), strict, 0.0)
    for low, high in ((1, 4), (4, 7)):
        near = halves(out)
        off = jnp.where(same(high) & ~same(low), strict, 0.0)
        power = dot(near, off)
        both = dot(power, jnp.concatenate([power, out], 1))
        power, out = both[:, :TOK], out - both[:, TOK:]
        both = dot(power, jnp.concatenate([power, out], 1))
        power, out = both[:, :TOK], out + both[:, TOK:]
        out = out + dot(power, out)
    return out


def chunk_kernel(
    proj_ref,
    gate_rows_ref,
    out_ref,
    saved_ref,
):
    row, col = iotas()
    grown, rest, total, write, ratio, _ = gates(gate_rows_ref, row, col)
    queries = unit(proj_ref[0].astype(F32))[0] * SCALE
    keys = unit(proj_ref[1].astype(F32))[0]
    values = proj_ref[2].astype(F32)
    out_grad = proj_ref[3].astype(F32)
    inner = dot(jnp.concatenate([keys, queries], 0), keys, NT)
    bare = jnp.where(row > col, ratio * inner[:TOK], 0.0)
    attend = ratio * inner[TOK:]
    inverse = inverse_of(bare * write, row, col)
    attended = dot(attend, out_grad, TN)
    direct = dot(out_grad, grown * queries, TN)
    solved = dot(inverse, jnp.concatenate([(write * grown) * keys, write * values], 1))
    key_weights, base = solved[:, :DK], solved[:, DK:]
    rest_keys = rest * keys
    moved = dot(solved, rest_keys, TN)
    eye = jnp.where(row == col, 1.0, 0.0).astype(F32)
    step = total * eye - moved[:DK]
    back = direct - dot(attended, key_weights, TN)
    for peer in range(COLS):
        out_ref[peer, :DK] = step
        out_ref[peer, DK : DK + SLICE] = moved[DK + peer * SLICE : DK + (peer + 1) * SLICE]
        out_ref[peer, DK + SLICE :] = back[peer * SLICE : (peer + 1) * SLICE]
    saved_ref[0] = inverse.T
    saved_ref[1] = key_weights
    saved_ref[2] = base
    saved_ref[3] = attend
    saved_ref[4] = bare
    saved_ref[5] = attended


def row_kernel(in_ref, out_ref, own_ref, scratch_ref):
    here_x = lax.axis_index("x")
    here_y = lax.axis_index("y")
    step = [in_ref[j, :DK] for j in range(COLS)]
    ahead = [in_ref[j, DK : DK + SLICE] for j in range(COLS)]
    back = [in_ref[j, DK + SLICE :] for j in range(COLS)]

    def joined(first, second):
        both = dot(jnp.concatenate([first[0], first[1]], 0), second[0])
        return (both[:DK], both[DK:] + second[1], first[2] + dot(second[2], first[0], NT))

    ones = list(zip(step, ahead, back))
    pairs = [joined(ones[2 * i], ones[2 * i + 1]) for i in range(4)]
    quads = [joined(pairs[2 * i], pairs[2 * i + 1]) for i in range(2)]
    whole = joined(quads[0], quads[1])

    zero = jnp.zeros((SLICE, DK), F32)
    b4 = quads[0][1]
    b2 = pairs[0][1]
    b6 = dot(b4, pairs[2][0]) + pairs[2][1]
    prefix = [
        zero,
        ahead[0],
        b2,
        dot(b2, step[2]) + ahead[2],
        b4,
        dot(b4, step[4]) + ahead[4],
        b6,
        dot(b6, step[6]) + ahead[6],
    ]
    c3 = quads[1][2]
    c5 = pairs[3][2]
    c1 = dot(c3, pairs[1][0], NT) + pairs[1][2]
    suffix = [
        dot(c1, step[1], NT) + back[1],
        c1,
        dot(c3, step[3], NT) + back[3],
        c3,
        dot(c5, step[5], NT) + back[5],
        c5,
        back[7],
        zero,
    ]

    row, col = iotas()
    eye = jnp.where(row == col, 1.0, 0.0).astype(F32)
    at_y = jnp.full((DK, DK), here_y, jnp.int32)
    high = at_y >= 4
    mid = (at_y & 2) != 0
    low = (at_y & 1) != 0
    before = jnp.where(high, quads[0][0], eye)
    before = dot(before, jnp.where(mid, jnp.where(high, pairs[2][0], pairs[0][0]), eye))
    single = in_ref[jnp.maximum(here_y - 1, 0), :DK]
    own_ref[0] = dot(before, jnp.where(low, single, eye))
    after = jnp.where(high, eye, quads[1][0])
    after = dot(jnp.where(mid, eye, jnp.where(high, pairs[3][0], pairs[1][0])), after)
    single = in_ref[jnp.minimum(here_y + 1, COLS - 1), :DK]
    own_ref[1] = dot(jnp.where(low, eye, single), after)

    scratch_ref[...] = whole[0]
    piece = scratch_ref[pl.ds(pl.multiple_of(here_y * SLICE, SLICE), SLICE)]
    at_x = jnp.full((SLICE, DK), here_x, jnp.int32)
    for peer_x in range(ROWS):
        own = at_x == peer_x
        sent = jnp.where(at_x < peer_x, whole[1], whole[2])
        for peer_y in range(COLS):
            slot = (COLS - 1 - peer_y) * ROWS + peer_x
            out_ref[slot, :SLICE] = jnp.where(own, prefix[peer_y], piece)
            out_ref[slot, SLICE:] = jnp.where(own, suffix[peer_y], sent)


def grad_kernel(
    proj_ref,
    gate_rows_ref,
    weight_ref,
    gate_ref,
    saved_ref,
    own_ref,
    in_ref,
    send_ref,
    low_ref,
    slope_ref,
):
    here_x = lax.axis_index("x")
    here_c = lax.axis_index("c")

    def part(row_at, kind):
        span = slice(kind * SLICE, (kind + 1) * SLICE)
        slots = [(COLS - 1 - y) * ROWS + row_at for y in range(COLS)]
        return jnp.concatenate([in_ref[slot, span] for slot in slots], 0)

    step1, step2 = halves(part(1, 0)), halves(part(2, 0))
    s1 = part(0, 1)
    s2 = dot(s1, step1) + part(1, 1)
    s3 = dot(s2, step2) + part(2, 1)
    g2 = part(3, 1)
    g1 = dot(g2, step2, NT) + part(2, 1)
    g0 = dot(g1, step1, NT) + part(1, 1)
    zero = jnp.zeros((DK, DK), F32)
    s_row = jnp.where(here_x == 0, zero, jnp.where(here_x == 1, s1, jnp.where(here_x == 2, s2, s3)))
    g_row = jnp.where(here_x == 3, zero, jnp.where(here_x == 2, g2, jnp.where(here_x == 1, g1, g0)))
    state = halves(dot(s_row, own_ref[0]) + part(here_x, 0))
    later = halves(dot(g_row, own_ref[1], NT) + part(here_x, 1))

    row, col = iotas()
    grown, rest, total, write, ratio, slope = gates(gate_rows_ref, row, col)
    q_unit, q_scale = unit(proj_ref[0].astype(F32))
    queries = q_unit * SCALE
    keys, k_scale = unit(proj_ref[1].astype(F32))
    values = proj_ref[2].astype(F32)
    out_grad = proj_ref[3].astype(F32)
    rest_keys = rest * keys
    attend = saved_ref[3]
    bare = saved_ref[4]

    fresh = halves(saved_ref[2] - dot(saved_ref[1], state, NT))
    d_fresh = saved_ref[5] + dot(rest_keys, later, NT)
    pulled = dot(saved_ref[0], d_fresh)
    both = dot(jnp.concatenate([out_grad, pulled], 0), state)
    d_query_decayed = both[:TOK]
    d_weighted = -both[TOK:]
    d_rest = dot(fresh, later)
    both = dot(jnp.concatenate([out_grad, pulled], 0), fresh, NT)
    d_attend = jnp.where(row >= col, both[:TOK], 0.0)
    d_lower = jnp.where(row > col, -both[TOK:], 0.0)
    d_qk = d_attend * ratio
    d_kk = d_lower * ratio * write
    stacked = jnp.concatenate([d_qk, d_kk], 0)
    by_key = dot(stacked, keys)
    across = dot(stacked, jnp.concatenate([queries, keys], 0), TN)
    d_queries = grown * d_query_decayed + by_key[:TOK]
    d_keys = by_key[TOK:] + across + rest * d_rest + (write * grown) * d_weighted

    lower_hit = d_lower * bare
    ratio_hit = d_attend * attend + lower_hit * write
    weighted_hit = grown * lane_sum(d_weighted * keys)
    rest_hit = lane_sum(d_rest * rest_keys)
    d_write = lane_sum(pulled * values) + weighted_hit + lane_sum(lower_hit)
    d_cumul = (
        lane_sum(ratio_hit)
        + grown * lane_sum(d_query_decayed * queries)
        - rest_hit
        + write * weighted_hit
    )
    d_cumul_row = jnp.sum(jnp.where(row == col, d_cumul, 0.0) - ratio_hit, axis=0, keepdims=True)
    at_end = jnp.sum(rest_hit, axis=0, keepdims=True) + total * jnp.sum(
        lane_sum(whole(later) * whole(state)), axis=0, keepdims=True
    )
    d_decay = lane_sum(jnp.where(col >= row, d_cumul_row, 0.0)) + at_end
    d_logit0 = d_decay * slope
    d_logit1 = d_write * write * (1.0 - write)

    d_queries = d_queries * SCALE
    grad_q = q_scale * (d_queries - q_unit * lane_sum(q_unit * d_queries))
    grad_k = k_scale * (d_keys - keys * lane_sum(keys * d_keys))
    grad_v = write * pulled
    low = [grad.astype(BF16) for grad in (grad_q, grad_k, grad_v)]
    for source in range(3):
        low_ref[source] = low[source]
    slopes = (d_logit0, d_logit1)
    slope_ref[...] = jnp.where(col == 0, d_logit0, d_logit1)
    for slot, peer in enumerate(ORDER):
        send_ref[slot] = projected_to(2 * peer + 1 - here_c, low, slopes, weight_ref, gate_ref)


def projected_to(head, low, slopes, weight_ref, gate_ref):
    at = pl.multiple_of(head * DK, DK)
    rows = pl.ds(at, DK)
    weights = jnp.concatenate([weight_ref[0, rows], weight_ref[1, rows]], 1)
    acc = lax.dot_general(
        jnp.concatenate(low[:2], 1), weights, NT, preferred_element_type=F32
    ) + lax.dot_general(low[2], weight_ref[2, rows], NT, preferred_element_type=F32)
    for kind in range(2):
        acc = acc + slopes[kind] * gate_ref[kind : kind + 1, rows].astype(F32)
    return acc


def keep_kernel(low_ref, slope_ref, weight_ref, gate_ref, other_ref, out_ref):
    here_c = lax.axis_index("c")
    low = [low_ref[source] for source in range(3)]
    slopes = (slope_ref[:, 0:1], slope_ref[:, 1:2])
    for slot, peer in enumerate(ORDER):
        own = projected_to(2 * peer + here_c, low, slopes, weight_ref, gate_ref)
        out_ref[slot] = other_ref[slot] + own


VMEM = pl.BlockSpec(memory_space=pltpu.VMEM)


def like(*shape):
    return jax.ShapeDtypeStruct(shape, F32)


def call(kernel, name, out_shape, in_specs, *args, scratch=()):
    return pl.pallas_call(
        kernel,
        out_shape=out_shape,
        in_specs=in_specs,
        out_specs=jax.tree.map(lambda _: VMEM, out_shape),
        scratch_shapes=scratch,
        compiler_params=pltpu.CompilerParams(vmem_limit_bytes=16 << 20),
        name=name,
    )(*args)


def shards(projected, out_grad, logits, head_params, qkv_weight, gate_weight):
    packed = jnp.concatenate([projected, out_grad[None]], 0)
    padded = jnp.pad(head_params.T, ((0, 0), (0, TOK - 2)))
    gate_rows = jnp.concatenate([logits[:, 0], padded], 0)
    gate = jnp.transpose(gate_weight, (1, 0, 2))[0]
    chunks, saved = call(
        chunk_kernel,
        "chunk",
        (like(COLS, DK + 2 * SLICE, DK), like(6, DK, DK)),
        [VMEM] * 2,
        packed,
        gate_rows,
    )
    chunks = lax.all_to_all(chunks, "y", 0, 0, tiled=True)
    rows, own = call(
        row_kernel,
        "row",
        (like(ROWS * COLS, 2 * SLICE, DK), like(2, DK, DK)),
        [VMEM],
        chunks,
        scratch=[pltpu.VMEM((DK, DK), F32)],
    )
    rows = lax.all_to_all(
        rows, ("x", "y"), 0, 0, tiled=True, axis_index_groups=[list(GRID_ORDER)]
    )
    send, low, slopes = call(
        grad_kernel,
        "grad",
        (
            like(COLS, TOK, DK),
            jax.ShapeDtypeStruct((3, TOK, DK), BF16),
            like(TOK, DK),
        ),
        [VMEM] * 7,
        packed,
        gate_rows,
        qkv_weight,
        gate,
        saved,
        own,
        rows,
    )
    other = lax.ppermute(send, "c", [(0, 1), (1, 0)])
    part = call(
        keep_kernel,
        "keep",
        like(COLS, TOK, DK),
        [VMEM] * 5,
        low,
        slopes,
        qkv_weight,
        gate,
        other,
    )
    summed = lax.all_to_all(
        part, "z", 0, 0, tiled=True, axis_index_groups=[list(ORDER)]
    )
    return summed.sum(axis=0).astype(BF16)


def solution(mesh):
    split = Mesh(mesh.devices.reshape(4, 8, 8, 2), ("x", "y", "z", "c"))
    seq, head = ("x", "y"), ("z", "c")
    in_specs = (
        P(None, seq, head),
        P(seq, head),
        P(None, head, seq),
        P(None, head),
        P(None, None, head),
        P(None, head, None),
    )
    return jax.shard_map(
        shards, mesh=split, in_specs=in_specs, out_specs=P(seq, head), check_vma=False
    )
```

```python
import jax
import jax.numpy as jnp
from jax import lax
from jax.experimental import pallas as pl
from jax.experimental.pallas import tpu as pltpu
from jax.sharding import Mesh
from jax.sharding import PartitionSpec as P

DK = 128
TOK = 128
ROWS = 4
COLS = 8
SLICE = DK // COLS
ORDER = (7, 5, 3, 6, 4, 2, 1, 0)
GRID_ORDER = tuple(x * COLS + y for y in reversed(range(COLS)) for x in range(ROWS))
SCALE = DK ** (-0.5)
F32 = jnp.float32

NN = (((1,), (0,)), ((), ()))
NT = (((1,), (1,)), ((), ()))
TN = (((0,), (0,)), ((), ()))


BF16 = jnp.bfloat16


def halves(x):
    if isinstance(x, tuple):
        return x
    high = x.astype(BF16)
    return high, (x - high.astype(F32)).astype(BF16)


def whole(pair):
    return pair[0].astype(F32) + pair[1].astype(F32)


def dot(left, right, dims=NN):
    (lh, ll), (rh, rl) = halves(left), halves(right)
    (lk,), (rk,) = dims[0]
    both = jnp.concatenate([lh, ll], lk)
    if rh.shape[1 - rk] == DK:
        first = jnp.concatenate([rh, rh], rk)
        second = jnp.concatenate([rl, jnp.zeros_like(rl)], rk)
        out = lax.dot_general(
            both, jnp.concatenate([first, second], 1 - rk), dims, preferred_element_type=F32
        )
        return out[:, :DK] + out[:, DK:]
    out = lax.dot_general(both, jnp.concatenate([rh, rh], rk), dims, preferred_element_type=F32)
    return out + lax.dot_general(lh, rl, dims, preferred_element_type=F32)


def iotas():
    row = lax.broadcasted_iota(jnp.int32, (TOK, TOK), 0)
    col = lax.broadcasted_iota(jnp.int32, (TOK, TOK), 1)
    return row, col


def lane_sum(x):
    return jnp.sum(x, axis=1, keepdims=True)


def unit(raw):
    scale = lax.rsqrt(lane_sum(raw * raw) + 1.0)
    return raw * scale, scale


def gates(gate_rows_ref, row, col):
    rows = gate_rows_ref[...]
    rate = jnp.exp(rows[2:3, 0:1])
    shifted = rows[0:1] + rows[2:3, 1:2]
    soft = jnp.maximum(shifted, 0.0) + jnp.log1p(jnp.exp(-jnp.abs(shifted)))
    decay_row = -rate * soft
    cumul = lane_sum(jnp.where(col <= row, decay_row, 0.0))
    cumul_row = jnp.sum(jnp.where(row == col, cumul, 0.0), axis=0, keepdims=True)
    last = cumul_row[:, TOK - 1 :]
    write = lane_sum(jnp.where(row == col, jax.nn.sigmoid(rows[1:2]), 0.0))
    lower = row >= col
    ratio = jnp.where(lower, jnp.exp(jnp.where(lower, cumul - cumul_row, 0.0)), 0.0)
    slope = lane_sum(jnp.where(row == col, -rate * jax.nn.sigmoid(shifted), 0.0))
    return jnp.exp(cumul), jnp.exp(last - cumul), jnp.exp(last), write, ratio, slope


def inverse_of(strict, given, row, col):
    eye = jnp.where(row == col, 1.0, 0.0).astype(F32)

    def same(level):
        return (row >> level) == (col >> level)

    out = eye - jnp.where(same(1), strict, 0.0)
    for low, high in ((1, 4), (4, 7)):
        off = jnp.where(same(high) & ~same(low), strict, 0.0)
        if high == 7:
            first = dot(out, jnp.concatenate([off, given], 1))
            power, out = first[:, :TOK], jnp.concatenate([out, first[:, TOK:]], 1)
        else:
            power = dot(out, off)
        both = dot(power, jnp.concatenate([power, out], 1))
        power, out = both[:, :TOK], out - both[:, TOK:]
        both = dot(power, jnp.concatenate([power, out], 1))
        power, out = both[:, :TOK], out + both[:, TOK:]
        out = out + dot(power, out)
    return out[:, :TOK], out[:, TOK:]


def chunk_kernel(
    proj_ref,
    gate_rows_ref,
    out_ref,
    saved_ref,
):
    row, col = iotas()
    grown, rest, total, write, ratio, _ = gates(gate_rows_ref, row, col)
    queries = unit(proj_ref[0].astype(F32))[0] * SCALE
    keys = unit(proj_ref[1].astype(F32))[0]
    values = proj_ref[2].astype(F32)
    out_grad = proj_ref[3].astype(F32)
    inner = dot(jnp.concatenate([keys, queries], 0), keys, NT)
    bare = jnp.where(row > col, ratio * inner[:TOK], 0.0)
    attend = ratio * inner[TOK:]
    given = jnp.concatenate([(write * grown) * keys, write * values], 1)
    inverse, solved = inverse_of(bare * write, given, row, col)
    attended = dot(attend, out_grad, TN)
    direct = dot(out_grad, grown * queries, TN)
    key_weights, base = solved[:, :DK], solved[:, DK:]
    rest_keys = rest * keys
    moved = dot(solved, rest_keys, TN)
    eye = jnp.where(row == col, 1.0, 0.0).astype(F32)
    step = total * eye - moved[:DK]
    back = direct - dot(attended, key_weights, TN)
    for peer in range(COLS):
        out_ref[peer, :DK] = step
        out_ref[peer, DK : DK + SLICE] = moved[DK + peer * SLICE : DK + (peer + 1) * SLICE]
        out_ref[peer, DK + SLICE :] = back[peer * SLICE : (peer + 1) * SLICE]
    saved_ref[0] = inverse.T
    saved_ref[1] = key_weights
    saved_ref[2] = base
    saved_ref[3] = attend
    saved_ref[4] = bare
    saved_ref[5] = attended


def row_kernel(in_ref, out_ref, own_ref, scratch_ref):
    here_x = lax.axis_index("x")
    here_y = lax.axis_index("y")
    step = [in_ref[j, :DK] for j in range(COLS)]
    ahead = [in_ref[j, DK : DK + SLICE] for j in range(COLS)]
    back = [in_ref[j, DK + SLICE :] for j in range(COLS)]

    def joined(first, second):
        both = dot(jnp.concatenate([first[0], first[1]], 0), second[0])
        return (both[:DK], both[DK:] + second[1], first[2] + dot(second[2], first[0], NT))

    ones = list(zip(step, ahead, back))
    pairs = [joined(ones[2 * i], ones[2 * i + 1]) for i in range(4)]
    quads = [joined(pairs[2 * i], pairs[2 * i + 1]) for i in range(2)]
    whole = joined(quads[0], quads[1])

    zero = jnp.zeros((SLICE, DK), F32)
    b4 = quads[0][1]
    b2 = pairs[0][1]
    b6 = dot(b4, pairs[2][0]) + pairs[2][1]
    prefix = [
        zero,
        ahead[0],
        b2,
        dot(b2, step[2]) + ahead[2],
        b4,
        dot(b4, step[4]) + ahead[4],
        b6,
        dot(b6, step[6]) + ahead[6],
    ]
    c3 = quads[1][2]
    c5 = pairs[3][2]
    c1 = dot(c3, pairs[1][0], NT) + pairs[1][2]
    suffix = [
        dot(c1, step[1], NT) + back[1],
        c1,
        dot(c3, step[3], NT) + back[3],
        c3,
        dot(c5, step[5], NT) + back[5],
        c5,
        back[7],
        zero,
    ]

    row, col = iotas()
    eye = jnp.where(row == col, 1.0, 0.0).astype(F32)
    at_y = jnp.full((DK, DK), here_y, jnp.int32)
    high = at_y >= 4
    mid = (at_y & 2) != 0
    low = (at_y & 1) != 0
    before = jnp.where(high, quads[0][0], eye)
    before = dot(before, jnp.where(mid, jnp.where(high, pairs[2][0], pairs[0][0]), eye))
    single = in_ref[jnp.maximum(here_y - 1, 0), :DK]
    own_ref[0] = dot(before, jnp.where(low, single, eye))
    after = jnp.where(high, eye, quads[1][0])
    after = dot(jnp.where(mid, eye, jnp.where(high, pairs[3][0], pairs[1][0])), after)
    single = in_ref[jnp.minimum(here_y + 1, COLS - 1), :DK]
    own_ref[1] = dot(jnp.where(low, eye, single), after)

    scratch_ref[...] = whole[0]
    piece = scratch_ref[pl.ds(pl.multiple_of(here_y * SLICE, SLICE), SLICE)]
    at_x = jnp.full((SLICE, DK), here_x, jnp.int32)
    for peer_x in range(ROWS):
        own = at_x == peer_x
        sent = jnp.where(at_x < peer_x, whole[1], whole[2])
        for peer_y in range(COLS):
            slot = (COLS - 1 - peer_y) * ROWS + peer_x
            out_ref[slot, :SLICE] = jnp.where(own, prefix[peer_y], piece)
            out_ref[slot, SLICE:] = jnp.where(own, suffix[peer_y], sent)


def grad_kernel(
    proj_ref,
    gate_rows_ref,
    weight_ref,
    gate_ref,
    saved_ref,
    own_ref,
    in_ref,
    send_ref,
    low_ref,
    slope_ref,
):
    here_x = lax.axis_index("x")
    here_c = lax.axis_index("c")

    def part(row_at, kind):
        span = slice(kind * SLICE, (kind + 1) * SLICE)
        slots = [(COLS - 1 - y) * ROWS + row_at for y in range(COLS)]
        return jnp.concatenate([in_ref[slot, span] for slot in slots], 0)

    step1, step2 = halves(part(1, 0)), halves(part(2, 0))
    s1 = part(0, 1)
    s2 = dot(s1, step1) + part(1, 1)
    s3 = dot(s2, step2) + part(2, 1)
    g2 = part(3, 1)
    g1 = dot(g2, step2, NT) + part(2, 1)
    g0 = dot(g1, step1, NT) + part(1, 1)
    zero = jnp.zeros((DK, DK), F32)
    s_row = jnp.where(here_x == 0, zero, jnp.where(here_x == 1, s1, jnp.where(here_x == 2, s2, s3)))
    g_row = jnp.where(here_x == 3, zero, jnp.where(here_x == 2, g2, jnp.where(here_x == 1, g1, g0)))
    state = halves(dot(s_row, own_ref[0]) + part(here_x, 0))
    later = halves(dot(g_row, own_ref[1], NT) + part(here_x, 1))

    row, col = iotas()
    grown, rest, total, write, ratio, slope = gates(gate_rows_ref, row, col)
    q_unit, q_scale = unit(proj_ref[0].astype(F32))
    queries = q_unit * SCALE
    keys, k_scale = unit(proj_ref[1].astype(F32))
    values = proj_ref[2].astype(F32)
    out_grad = proj_ref[3].astype(F32)
    rest_keys = rest * keys
    attend = saved_ref[3]
    bare = saved_ref[4]

    fresh = halves(saved_ref[2] - dot(saved_ref[1], state, NT))
    d_fresh = saved_ref[5] + dot(rest_keys, later, NT)
    pulled = dot(saved_ref[0], d_fresh)
    both = dot(jnp.concatenate([out_grad, pulled], 0), state)
    d_query_decayed = both[:TOK]
    d_weighted = -both[TOK:]
    d_rest = dot(fresh, later)
    both = dot(jnp.concatenate([out_grad, pulled], 0), fresh, NT)
    d_attend = jnp.where(row >= col, both[:TOK], 0.0)
    d_lower = jnp.where(row > col, -both[TOK:], 0.0)
    d_qk = d_attend * ratio
    d_kk = d_lower * ratio * write
    stacked = jnp.concatenate([d_qk, d_kk], 0)
    by_key = dot(stacked, keys)
    across = dot(stacked, jnp.concatenate([queries, keys], 0), TN)
    d_queries = grown * d_query_decayed + by_key[:TOK]
    d_keys = by_key[TOK:] + across + rest * d_rest + (write * grown) * d_weighted

    lower_hit = d_lower * bare
    ratio_hit = d_attend * attend + lower_hit * write
    weighted_hit = grown * lane_sum(d_weighted * keys)
    rest_hit = lane_sum(d_rest * rest_keys)
    d_write = lane_sum(pulled * values) + weighted_hit + lane_sum(lower_hit)
    d_cumul = (
        lane_sum(ratio_hit)
        + grown * lane_sum(d_query_decayed * queries)
        - rest_hit
        + write * weighted_hit
    )
    d_cumul_row = jnp.sum(jnp.where(row == col, d_cumul, 0.0) - ratio_hit, axis=0, keepdims=True)
    at_end = jnp.sum(rest_hit, axis=0, keepdims=True) + total * jnp.sum(
        lane_sum(whole(later) * whole(state)), axis=0, keepdims=True
    )
    d_decay = lane_sum(jnp.where(col >= row, d_cumul_row, 0.0)) + at_end
    d_logit0 = d_decay * slope
    d_logit1 = d_write * write * (1.0 - write)

    d_queries = d_queries * SCALE
    grad_q = q_scale * (d_queries - q_unit * lane_sum(q_unit * d_queries))
    grad_k = k_scale * (d_keys - keys * lane_sum(keys * d_keys))
    grad_v = write * pulled
    low = [grad.astype(BF16) for grad in (grad_q, grad_k, grad_v)]
    for source in range(3):
        low_ref[source] = low[source]
    slopes = (d_logit0, d_logit1)
    slope_ref[...] = jnp.where(col == 0, d_logit0, d_logit1)
    for slot, peer in enumerate(ORDER):
        send_ref[slot] = projected_to(2 * peer + 1 - here_c, low, slopes, weight_ref, gate_ref)


def projected_to(head, low, slopes, weight_ref, gate_ref):
    at = pl.multiple_of(head * DK, DK)
    rows = pl.ds(at, DK)
    weights = jnp.concatenate([weight_ref[0, rows], weight_ref[1, rows]], 1)
    acc = lax.dot_general(
        jnp.concatenate(low[:2], 1), weights, NT, preferred_element_type=F32
    ) + lax.dot_general(low[2], weight_ref[2, rows], NT, preferred_element_type=F32)
    for kind in range(2):
        acc = acc + slopes[kind] * gate_ref[kind : kind + 1, rows].astype(F32)
    return acc


def keep_kernel(low_ref, slope_ref, weight_ref, gate_ref, out_ref):
    here_c = lax.axis_index("c")
    low = [low_ref[source] for source in range(3)]
    slopes = (slope_ref[:, 0:1], slope_ref[:, 1:2])
    for slot, peer in enumerate(ORDER):
        out_ref[slot] = projected_to(2 * peer + here_c, low, slopes, weight_ref, gate_ref)


VMEM = pl.BlockSpec(memory_space=pltpu.VMEM)


def like(*shape):
    return jax.ShapeDtypeStruct(shape, F32)


def call(kernel, name, out_shape, in_specs, *args, scratch=()):
    return pl.pallas_call(
        kernel,
        out_shape=out_shape,
        in_specs=in_specs,
        out_specs=jax.tree.map(lambda _: VMEM, out_shape),
        scratch_shapes=scratch,
        compiler_params=pltpu.CompilerParams(vmem_limit_bytes=16 << 20),
        name=name,
    )(*args)


def shards(projected, out_grad, logits, head_params, qkv_weight, gate_weight):
    packed = jnp.concatenate([projected, out_grad[None]], 0)
    padded = jnp.pad(head_params.T, ((0, 0), (0, TOK - 2)))
    gate_rows = jnp.concatenate([logits[:, 0], padded], 0)
    gate = jnp.transpose(gate_weight, (1, 0, 2))[0]
    chunks, saved = call(
        chunk_kernel,
        "chunk",
        (like(COLS, DK + 2 * SLICE, DK), like(6, DK, DK)),
        [VMEM] * 2,
        packed,
        gate_rows,
    )
    chunks = lax.all_to_all(chunks, "y", 0, 0, tiled=True)
    rows, own = call(
        row_kernel,
        "row",
        (like(ROWS * COLS, 2 * SLICE, DK), like(2, DK, DK)),
        [VMEM],
        chunks,
        scratch=[pltpu.VMEM((DK, DK), F32)],
    )
    rows = lax.all_to_all(
        rows, ("x", "y"), 0, 0, tiled=True, axis_index_groups=[list(GRID_ORDER)]
    )
    send, low, slopes = call(
        grad_kernel,
        "grad",
        (
            like(COLS, TOK, DK),
            jax.ShapeDtypeStruct((3, TOK, DK), BF16),
            like(TOK, DK),
        ),
        [VMEM] * 7,
        packed,
        gate_rows,
        qkv_weight,
        gate,
        saved,
        own,
        rows,
    )
    other = lax.ppermute(send, "c", [(0, 1), (1, 0)])
    part = call(
        keep_kernel,
        "keep",
        like(COLS, TOK, DK),
        [VMEM] * 4,
        low,
        slopes,
        qkv_weight,
        gate,
    )
    part = part + other
    summed = lax.all_to_all(
        part, "z", 0, 0, tiled=True, axis_index_groups=[list(ORDER)]
    )
    return summed.sum(axis=0).astype(BF16)


def solution(mesh):
    split = Mesh(mesh.devices.reshape(4, 8, 8, 2), ("x", "y", "z", "c"))
    seq, head = ("x", "y"), ("z", "c")
    in_specs = (
        P(None, seq, head),
        P(seq, head),
        P(None, head, seq),
        P(None, head),
        P(None, None, head),
        P(None, head, None),
    )
    return jax.shard_map(
        shards, mesh=split, in_specs=in_specs, out_specs=P(seq, head), check_vma=False
    )
```

```python
import jax
import jax.numpy as jnp
from jax import lax
from jax.experimental import pallas as pl
from jax.experimental.pallas import tpu as pltpu
from jax.sharding import Mesh
from jax.sharding import PartitionSpec as P

DK = 128
TOK = 128
ROWS = 4
COLS = 8
SLICE = DK // COLS
ORDER = (7, 6, 5, 4, 3, 2, 1, 0)
GRID_ORDER = tuple(x * COLS + y for y in reversed(range(COLS)) for x in range(ROWS))
SCALE = DK ** (-0.5)
F32 = jnp.float32

NN = (((1,), (0,)), ((), ()))
NT = (((1,), (1,)), ((), ()))
TN = (((0,), (0,)), ((), ()))


BF16 = jnp.bfloat16


def halves(x):
    if isinstance(x, tuple):
        return x
    high = x.astype(BF16)
    return high, (x - high.astype(F32)).astype(BF16)


def whole(pair):
    return pair[0].astype(F32) + pair[1].astype(F32)


def dot(left, right, dims=NN):
    (lh, ll), (rh, rl) = halves(left), halves(right)
    (lk,), (rk,) = dims[0]
    both = jnp.concatenate([lh, ll], lk)
    if rh.shape[1 - rk] == DK:
        first = jnp.concatenate([rh, rh], rk)
        second = jnp.concatenate([rl, jnp.zeros_like(rl)], rk)
        out = lax.dot_general(
            both, jnp.concatenate([first, second], 1 - rk), dims, preferred_element_type=F32
        )
        return out[:, :DK] + out[:, DK:]
    out = lax.dot_general(both, jnp.concatenate([rh, rh], rk), dims, preferred_element_type=F32)
    return out + lax.dot_general(lh, rl, dims, preferred_element_type=F32)


def iotas():
    row = lax.broadcasted_iota(jnp.int32, (TOK, TOK), 0)
    col = lax.broadcasted_iota(jnp.int32, (TOK, TOK), 1)
    return row, col


def lane_sum(x):
    return jnp.sum(x, axis=1, keepdims=True)


def unit(raw):
    scale = lax.rsqrt(lane_sum(raw * raw) + 1.0)
    return raw * scale, scale


def gates(gate_rows_ref, row, col):
    rows = gate_rows_ref[...]
    rate = jnp.exp(rows[2:3, 0:1])
    shifted = rows[0:1] + rows[2:3, 1:2]
    soft = jnp.maximum(shifted, 0.0) + jnp.log1p(jnp.exp(-jnp.abs(shifted)))
    decay_row = -rate * soft
    cumul = lane_sum(jnp.where(col <= row, decay_row, 0.0))
    cumul_row = jnp.sum(jnp.where(row == col, cumul, 0.0), axis=0, keepdims=True)
    last = cumul_row[:, TOK - 1 :]
    write = lane_sum(jnp.where(row == col, jax.nn.sigmoid(rows[1:2]), 0.0))
    lower = row >= col
    ratio = jnp.where(lower, jnp.exp(jnp.where(lower, cumul - cumul_row, 0.0)), 0.0)
    slope = lane_sum(jnp.where(row == col, -rate * jax.nn.sigmoid(shifted), 0.0))
    return jnp.exp(cumul), jnp.exp(last - cumul), jnp.exp(last), write, ratio, slope


def inverse_of(strict, given, row, col):
    eye = jnp.where(row == col, 1.0, 0.0).astype(F32)

    def same(level):
        return (row >> level) == (col >> level)

    out = eye - jnp.where(same(1), strict, 0.0)
    for low, high in ((1, 4), (4, 7)):
        off = jnp.where(same(high) & ~same(low), strict, 0.0)
        if high == 7:
            first = dot(out, jnp.concatenate([off, given], 1))
            power, out = first[:, :TOK], jnp.concatenate([out, first[:, TOK:]], 1)
        else:
            power = dot(out, off)
        both = dot(power, jnp.concatenate([power, out], 1))
        power, out = both[:, :TOK], out - both[:, TOK:]
        both = dot(power, jnp.concatenate([power, out], 1))
        power, out = both[:, :TOK], out + both[:, TOK:]
        out = out + dot(power, out)
    return out[:, :TOK], out[:, TOK:]


def chunk_kernel(
    proj_ref,
    gate_rows_ref,
    out_ref,
    saved_ref,
):
    row, col = iotas()
    grown, rest, total, write, ratio, _ = gates(gate_rows_ref, row, col)
    queries = unit(proj_ref[0].astype(F32))[0] * SCALE
    keys = unit(proj_ref[1].astype(F32))[0]
    values = proj_ref[2].astype(F32)
    out_grad = proj_ref[3].astype(F32)
    inner = dot(jnp.concatenate([keys, queries], 0), keys, NT)
    bare = jnp.where(row > col, ratio * inner[:TOK], 0.0)
    attend = ratio * inner[TOK:]
    given = jnp.concatenate([(write * grown) * keys, write * values], 1)
    inverse, solved = inverse_of(bare * write, given, row, col)
    attended = dot(attend, out_grad, TN)
    direct = dot(out_grad, grown * queries, TN)
    key_weights, base = solved[:, :DK], solved[:, DK:]
    rest_keys = rest * keys
    moved = dot(solved, rest_keys, TN)
    eye = jnp.where(row == col, 1.0, 0.0).astype(F32)
    step = total * eye - moved[:DK]
    back = direct - dot(attended, key_weights, TN)
    for peer in range(COLS):
        out_ref[peer, :DK] = step
        out_ref[peer, DK : DK + SLICE] = moved[DK + peer * SLICE : DK + (peer + 1) * SLICE]
        out_ref[peer, DK + SLICE :] = back[peer * SLICE : (peer + 1) * SLICE]
    saved_ref[0] = inverse.T
    saved_ref[1] = key_weights
    saved_ref[2] = base
    saved_ref[3] = attend
    saved_ref[4] = bare
    saved_ref[5] = attended


def row_kernel(in_ref, out_ref, own_ref, scratch_ref):
    here_x = lax.axis_index("x")
    here_y = lax.axis_index("y")
    step = [in_ref[j, :DK] for j in range(COLS)]
    ahead = [in_ref[j, DK : DK + SLICE] for j in range(COLS)]
    back = [in_ref[j, DK + SLICE :] for j in range(COLS)]

    def joined(first, second):
        both = dot(jnp.concatenate([first[0], first[1]], 0), second[0])
        return (both[:DK], both[DK:] + second[1], first[2] + dot(second[2], first[0], NT))

    ones = list(zip(step, ahead, back))
    pairs = [joined(ones[2 * i], ones[2 * i + 1]) for i in range(4)]
    quads = [joined(pairs[2 * i], pairs[2 * i + 1]) for i in range(2)]
    whole = joined(quads[0], quads[1])

    zero = jnp.zeros((SLICE, DK), F32)
    b4 = quads[0][1]
    b2 = pairs[0][1]
    b6 = dot(b4, pairs[2][0]) + pairs[2][1]
    prefix = [
        zero,
        ahead[0],
        b2,
        dot(b2, step[2]) + ahead[2],
        b4,
        dot(b4, step[4]) + ahead[4],
        b6,
        dot(b6, step[6]) + ahead[6],
    ]
    c3 = quads[1][2]
    c5 = pairs[3][2]
    c1 = dot(c3, pairs[1][0], NT) + pairs[1][2]
    suffix = [
        dot(c1, step[1], NT) + back[1],
        c1,
        dot(c3, step[3], NT) + back[3],
        c3,
        dot(c5, step[5], NT) + back[5],
        c5,
        back[7],
        zero,
    ]

    row, col = iotas()
    eye = jnp.where(row == col, 1.0, 0.0).astype(F32)
    at_y = jnp.full((DK, DK), here_y, jnp.int32)
    high = at_y >= 4
    mid = (at_y & 2) != 0
    low = (at_y & 1) != 0
    before = jnp.where(high, quads[0][0], eye)
    before = dot(before, jnp.where(mid, jnp.where(high, pairs[2][0], pairs[0][0]), eye))
    single = in_ref[jnp.maximum(here_y - 1, 0), :DK]
    own_ref[0] = dot(before, jnp.where(low, single, eye))
    after = jnp.where(high, eye, quads[1][0])
    after = dot(jnp.where(mid, eye, jnp.where(high, pairs[3][0], pairs[1][0])), after)
    single = in_ref[jnp.minimum(here_y + 1, COLS - 1), :DK]
    own_ref[1] = dot(jnp.where(low, eye, single), after)

    scratch_ref[...] = whole[0]
    piece = scratch_ref[pl.ds(pl.multiple_of(here_y * SLICE, SLICE), SLICE)]
    at_x = jnp.full((SLICE, DK), here_x, jnp.int32)
    for peer_x in range(ROWS):
        own = at_x == peer_x
        sent = jnp.where(at_x < peer_x, whole[1], whole[2])
        for peer_y in range(COLS):
            slot = (COLS - 1 - peer_y) * ROWS + peer_x
            out_ref[slot, :SLICE] = jnp.where(own, prefix[peer_y], piece)
            out_ref[slot, SLICE:] = jnp.where(own, suffix[peer_y], sent)


def grad_kernel(
    proj_ref,
    gate_rows_ref,
    weight_ref,
    gate_ref,
    saved_ref,
    own_ref,
    in_ref,
    send_ref,
    low_ref,
    slope_ref,
):
    here_x = lax.axis_index("x")
    here_c = lax.axis_index("c")

    def part(row_at, kind):
        span = slice(kind * SLICE, (kind + 1) * SLICE)
        slots = [(COLS - 1 - y) * ROWS + row_at for y in range(COLS)]
        return jnp.concatenate([in_ref[slot, span] for slot in slots], 0)

    step1, step2 = halves(part(1, 0)), halves(part(2, 0))
    s1 = part(0, 1)
    s2 = dot(s1, step1) + part(1, 1)
    s3 = dot(s2, step2) + part(2, 1)
    g2 = part(3, 1)
    g1 = dot(g2, step2, NT) + part(2, 1)
    g0 = dot(g1, step1, NT) + part(1, 1)
    zero = jnp.zeros((DK, DK), F32)
    s_row = jnp.where(here_x == 0, zero, jnp.where(here_x == 1, s1, jnp.where(here_x == 2, s2, s3)))
    g_row = jnp.where(here_x == 3, zero, jnp.where(here_x == 2, g2, jnp.where(here_x == 1, g1, g0)))
    state = halves(dot(s_row, own_ref[0]) + part(here_x, 0))
    later = halves(dot(g_row, own_ref[1], NT) + part(here_x, 1))

    row, col = iotas()
    grown, rest, total, write, ratio, slope = gates(gate_rows_ref, row, col)
    q_unit, q_scale = unit(proj_ref[0].astype(F32))
    queries = q_unit * SCALE
    keys, k_scale = unit(proj_ref[1].astype(F32))
    values = proj_ref[2].astype(F32)
    out_grad = proj_ref[3].astype(F32)
    rest_keys = rest * keys
    attend = saved_ref[3]
    bare = saved_ref[4]

    fresh = halves(saved_ref[2] - dot(saved_ref[1], state, NT))
    d_fresh = saved_ref[5] + dot(rest_keys, later, NT)
    pulled = dot(saved_ref[0], d_fresh)
    both = dot(jnp.concatenate([out_grad, pulled], 0), state)
    d_query_decayed = both[:TOK]
    d_weighted = -both[TOK:]
    d_rest = dot(fresh, later)
    both = dot(jnp.concatenate([out_grad, pulled], 0), fresh, NT)
    d_attend = jnp.where(row >= col, both[:TOK], 0.0)
    d_lower = jnp.where(row > col, -both[TOK:], 0.0)
    d_qk = d_attend * ratio
    d_kk = d_lower * ratio * write
    stacked = jnp.concatenate([d_qk, d_kk], 0)
    by_key = dot(stacked, keys)
    across = dot(stacked, jnp.concatenate([queries, keys], 0), TN)
    d_queries = grown * d_query_decayed + by_key[:TOK]
    d_keys = by_key[TOK:] + across + rest * d_rest + (write * grown) * d_weighted

    lower_hit = d_lower * bare
    ratio_hit = d_attend * attend + lower_hit * write
    weighted_hit = grown * lane_sum(d_weighted * keys)
    rest_hit = lane_sum(d_rest * rest_keys)
    d_write = lane_sum(pulled * values) + weighted_hit + lane_sum(lower_hit)
    d_cumul = (
        lane_sum(ratio_hit)
        + grown * lane_sum(d_query_decayed * queries)
        - rest_hit
        + write * weighted_hit
    )
    d_cumul_row = jnp.sum(jnp.where(row == col, d_cumul, 0.0) - ratio_hit, axis=0, keepdims=True)
    at_end = jnp.sum(rest_hit, axis=0, keepdims=True) + total * jnp.sum(
        lane_sum(whole(later) * whole(state)), axis=0, keepdims=True
    )
    d_decay = lane_sum(jnp.where(col >= row, d_cumul_row, 0.0)) + at_end
    d_logit0 = d_decay * slope
    d_logit1 = d_write * write * (1.0 - write)

    d_queries = d_queries * SCALE
    grad_q = q_scale * (d_queries - q_unit * lane_sum(q_unit * d_queries))
    grad_k = k_scale * (d_keys - keys * lane_sum(keys * d_keys))
    grad_v = write * pulled
    low = [grad.astype(BF16) for grad in (grad_q, grad_k, grad_v)]
    for source in range(3):
        low_ref[source] = low[source]
    slopes = (d_logit0, d_logit1)
    slope_ref[...] = jnp.where(col == 0, d_logit0, d_logit1)
    for slot, peer in enumerate(ORDER):
        send_ref[slot] = projected_to(2 * peer + 1 - here_c, low, slopes, weight_ref, gate_ref)


def projected_to(head, low, slopes, weight_ref, gate_ref):
    at = pl.multiple_of(head * DK, DK)
    rows = pl.ds(at, DK)
    weights = jnp.concatenate([weight_ref[0, rows], weight_ref[1, rows]], 1)
    acc = lax.dot_general(
        jnp.concatenate(low[:2], 1), weights, NT, preferred_element_type=F32
    ) + lax.dot_general(low[2], weight_ref[2, rows], NT, preferred_element_type=F32)
    for kind in range(2):
        acc = acc + slopes[kind] * gate_ref[kind : kind + 1, rows].astype(F32)
    return acc


def keep_kernel(low_ref, slope_ref, weight_ref, gate_ref, out_ref):
    here_c = lax.axis_index("c")
    low = [low_ref[source] for source in range(3)]
    slopes = (slope_ref[:, 0:1], slope_ref[:, 1:2])
    for slot, peer in enumerate(ORDER):
        out_ref[slot] = projected_to(2 * peer + here_c, low, slopes, weight_ref, gate_ref)


VMEM = pl.BlockSpec(memory_space=pltpu.VMEM)


def like(*shape):
    return jax.ShapeDtypeStruct(shape, F32)


def call(kernel, name, out_shape, in_specs, *args, scratch=()):
    return pl.pallas_call(
        kernel,
        out_shape=out_shape,
        in_specs=in_specs,
        out_specs=jax.tree.map(lambda _: VMEM, out_shape),
        scratch_shapes=scratch,
        compiler_params=pltpu.CompilerParams(vmem_limit_bytes=16 << 20),
        name=name,
    )(*args)


def shards(projected, out_grad, logits, head_params, qkv_weight, gate_weight):
    packed = jnp.concatenate([projected, out_grad[None]], 0)
    padded = jnp.pad(head_params.T, ((0, 0), (0, TOK - 2)))
    gate_rows = jnp.concatenate([logits[:, 0], padded], 0)
    gate = jnp.transpose(gate_weight, (1, 0, 2))[0]
    chunks, saved = call(
        chunk_kernel,
        "chunk",
        (like(COLS, DK + 2 * SLICE, DK), like(6, DK, DK)),
        [VMEM] * 2,
        packed,
        gate_rows,
    )
    chunks = lax.all_to_all(chunks, "y", 0, 0, tiled=True)
    rows, own = call(
        row_kernel,
        "row",
        (like(ROWS * COLS, 2 * SLICE, DK), like(2, DK, DK)),
        [VMEM],
        chunks,
        scratch=[pltpu.VMEM((DK, DK), F32)],
    )
    rows = lax.all_to_all(
        rows, ("x", "y"), 0, 0, tiled=True, axis_index_groups=[list(GRID_ORDER)]
    )
    send, low, slopes = call(
        grad_kernel,
        "grad",
        (
            like(COLS, TOK, DK),
            jax.ShapeDtypeStruct((3, TOK, DK), BF16),
            like(TOK, DK),
        ),
        [VMEM] * 7,
        packed,
        gate_rows,
        qkv_weight,
        gate,
        saved,
        own,
        rows,
    )
    other = lax.ppermute(send, "c", [(0, 1), (1, 0)])
    part = call(
        keep_kernel,
        "keep",
        like(COLS, TOK, DK),
        [VMEM] * 4,
        low,
        slopes,
        qkv_weight,
        gate,
    )
    part = part + other
    summed = lax.all_to_all(
        part, "z", 0, 0, tiled=True, axis_index_groups=[list(ORDER)]
    )
    return summed.sum(axis=0).astype(BF16)


def solution(mesh):
    split = Mesh(mesh.devices.reshape(4, 8, 8, 2), ("x", "y", "z", "c"))
    seq, head = ("x", "y"), ("z", "c")
    in_specs = (
        P(None, seq, head),
        P(seq, head),
        P(None, head, seq),
        P(None, head),
        P(None, None, head),
        P(None, head, None),
    )
    return jax.shard_map(
        shards, mesh=split, in_specs=in_specs, out_specs=P(seq, head), check_vma=False
    )
```
